32 devices in a mesh: dp: 2 (over x), tx: 4 (over z), ty: 4 (over y, core).
Axes of the slice: x: 2, y: 2, z: 4, core: 2. Of those that a mesh axis runs over, the one named last changes fastest.
Arguments:
- residual: float32 [256, 4096], P('dp', 'tx'), parts along dimension 0
- norm_w: float32 [2, 4096], P(None, 'tx')
- w_in: bfloat16 [2, 4096, 2, 8192], P(None, 'tx', None, 'ty')
- conv_w: float32 [2, 8192, 4], P(None, 'ty')
- conv_b: float32 [2, 8192], P(None, 'ty')
- w_x: bfloat16 [2, 8192, 288], P(None, 'ty')
- w_dt: bfloat16 [2, 256, 8192], P(None, None, 'ty')
- dt_bias: float32 [2, 8192], P(None, 'ty')
- a_log: float32 [2, 8192, 16], P(None, 'ty')
- d_skip: float32 [2, 8192], P(None, 'ty')
- w_out: bfloat16 [2, 8192, 4096], P(None, 'ty', 'tx')
- conv_state: bfloat16 [2, 256, 8192, 3], P(None, ('dp', 'tx'), 'ty'), parts along dimension 1
- ssm_state: float32 [2, 256, 8192, 16], P(None, ('dp', 'tx'), 'ty'), parts along dimension 1
Outputs:
- output 1: float32 [256, 4096], P('dp', 'tx'), parts along dimension 0
- output 2: bfloat16 [2, 256, 8192, 3], P(None, ('dp', 'tx'), 'ty'), parts along dimension 1
- output 3: float32 [2, 256, 8192, 16], P(None, ('dp', 'tx'), 'ty'), parts along dimension 1
There are 2 independent parts. The reference program is written for one: setup_inputs(seed, part) draws one part's arguments, and reference() takes and returns one part's arrays. A program takes and returns all parts, laid end to end along the dimension named above; an argument that names none is the same for every part.
All inputs are finite; a program needn't handle non-finite values.
Results may differ from the reference program's by a relative error of at most 0.0151635.
Values are sent between devices in bfloat16 or wider.
A program may use at most 1 GiB of HBM per device.

```python
import math
import jax
import jax.numpy as jnp
from jax import lax

BATCH_ROWS = 128
D_MODEL = 4096
D_INNER = 8192
D_STATE = 16
DT_RANK = 256
CONV_WIDTH = 4
LAYERS = 2
NORM_EPS = 1e-5
INNER_EPS = 1e-6


def setup_inputs(seed: int = 0, part: int = 0) -> dict:
    keys = jax.random.split(jax.random.key(seed), 10)
    row_keys = jax.random.split(jax.random.fold_in(jax.random.key(seed + 1), part), 3)
    col_pos = jnp.arange(D_MODEL, dtype=jnp.float32) / D_MODEL
    col_scale = jnp.exp(3.0 * col_pos - 1.5)
    residual = jax.random.normal(row_keys[0], (BATCH_ROWS, D_MODEL), jnp.float32) * col_scale
    norm_w = jax.random.uniform(keys[0], (LAYERS, D_MODEL), jnp.float32, 0.5, 1.5)
    w_in = (jax.random.normal(keys[1], (LAYERS, D_MODEL, 2, D_INNER), jnp.float32) * D_MODEL ** -0.5).astype(jnp.bfloat16)
    conv_w = jax.random.normal(keys[2], (LAYERS, D_INNER, CONV_WIDTH), jnp.float32) * CONV_WIDTH ** -0.5
    conv_b = jax.random.normal(keys[3], (LAYERS, D_INNER), jnp.float32) * 0.2
    w_x = (jax.random.normal(keys[4], (LAYERS, D_INNER, DT_RANK + 2 * D_STATE), jnp.float32) * D_INNER ** -0.5).astype(jnp.bfloat16)
    w_dt = (jax.random.normal(keys[5], (LAYERS, DT_RANK, D_INNER), jnp.float32) * DT_RANK ** -0.5).astype(jnp.bfloat16)
    dt_init = jnp.exp(jax.random.uniform(keys[6], (LAYERS, D_INNER), jnp.float32, math.log(0.005), math.log(0.1)))
    dt_bias = dt_init + jnp.log(-jnp.expm1(-dt_init))
    a_log = jnp.log(jax.random.uniform(keys[7], (LAYERS, D_INNER, D_STATE), jnp.float32, 1.0, 16.0))
    d_skip = jax.random.uniform(keys[8], (LAYERS, D_INNER), jnp.float32, 0.5, 2.0)
    w_out = (jax.random.normal(keys[9], (LAYERS, D_INNER, D_MODEL), jnp.float32) * D_INNER ** -0.5).astype(jnp.bfloat16)
    conv_state = jax.random.normal(row_keys[1], (LAYERS, BATCH_ROWS, D_INNER, CONV_WIDTH - 1), jnp.float32).astype(jnp.bfloat16)
    ssm_state = jax.random.normal(row_keys[2], (LAYERS, BATCH_ROWS, D_INNER, D_STATE), jnp.float32) * 0.5
    return {"residual": residual, "norm_w": norm_w, "w_in": w_in, "conv_w": conv_w, "conv_b": conv_b, "w_x": w_x, "w_dt": w_dt, "dt_bias": dt_bias, "a_log": a_log, "d_skip": d_skip, "w_out": w_out, "conv_state": conv_state, "ssm_state": ssm_state}


def unit_rms(vec):
    return vec * lax.rsqrt(jnp.mean(vec * vec, axis=-1, keepdims=True) + INNER_EPS)


def mixer_layer(residual, params):
    norm_w, w_in, conv_w, conv_b, w_x, w_dt, dt_bias, a_log, d_skip, w_out, conv_prev, ssm_prev = params
    variance = jnp.mean(residual * residual, axis=-1, keepdims=True)
    normed = (residual * lax.rsqrt(variance + NORM_EPS) * norm_w).astype(jnp.bfloat16)
    proj_in = jnp.dot(normed, w_in.reshape(D_MODEL, 2 * D_INNER), preferred_element_type=jnp.float32).astype(jnp.bfloat16)
    x_branch = proj_in[:, :D_INNER]
    z_branch = proj_in[:, D_INNER:]
    window = jnp.concatenate([conv_prev, x_branch[:, :, None]], axis=-1)
    conv_val = jnp.sum(window.astype(jnp.float32) * conv_w, axis=-1) + conv_b
    x_conv = jax.nn.silu(conv_val).astype(jnp.bfloat16)
    x_dbl = jnp.dot(x_conv, w_x, preferred_element_type=jnp.float32)
    dt_low = unit_rms(x_dbl[:, :DT_RANK])
    b_mat = unit_rms(x_dbl[:, DT_RANK:DT_RANK + D_STATE])
    c_mat = unit_rms(x_dbl[:, DT_RANK + D_STATE:])
    delta = jax.nn.softplus(jnp.dot(dt_low.astype(jnp.bfloat16), w_dt, preferred_element_type=jnp.float32) + dt_bias)
    x_float = x_conv.astype(jnp.float32)
    decay = jnp.exp(delta[:, :, None] * -jnp.exp(a_log))
    ssm_new = decay * ssm_prev + (delta * x_float)[:, :, None] * b_mat[:, None, :]
    state_val = jnp.sum(ssm_new * c_mat[:, None, :], axis=-1)
    gated = ((state_val + d_skip * x_float) * jax.nn.silu(z_branch.astype(jnp.float32))).astype(jnp.bfloat16)
    out_proj = jnp.dot(gated, w_out, preferred_element_type=jnp.float32)
    return residual + out_proj, (window[:, :, 1:], ssm_new)


def reference(residual, norm_w, w_in, conv_w, conv_b, w_x, w_dt, dt_bias, a_log, d_skip, w_out, conv_state, ssm_state):
    layer_params = (norm_w, w_in, conv_w, conv_b, w_x, w_dt, dt_bias, a_log, d_skip, w_out, conv_state, ssm_state)
    residual_out, caches = lax.scan(mixer_layer, residual, layer_params)
    return residual_out, caches[0], caches[1]
```

```python
import jax
import jax.numpy as jnp
from jax import lax
from jax.experimental import pallas as pl
from jax.experimental.pallas import tpu as pltpu
from jax.sharding import PartitionSpec as P

NORM_EPS = 1e-5
INNER_EPS = 1e-6
LOG2E = 1.4426950408889634
BF16, F32 = jnp.bfloat16, jnp.float32
MESH = pl.DeviceIdType.MESH
ANY = pl.BlockSpec(memory_space=pl.ANY)


def dot(a, b):
    return jnp.dot(a, b, preferred_element_type=F32)


def make_kernel(n_layer, n_tx, n_ty, rows, d_loc, chan, rank, n_state, chunk):
    blk = rows // n_tx
    half = rows // 2
    n_c = chan // chunk
    d_model = d_loc * n_tx
    n_q = 4
    qw = d_loc // n_q
    n_w = chan // 128
    last = n_tx - 1

    def kernel(
        r_hbm, nw_hbm, win_hbm, cw_hbm, cb_hbm, wx_hbm, wdt_hbm, db_hbm, al_hbm, ds_hbm, wout_hbm, cs_hbm, ss_hbm,
        r_out, conv_out, ssm_out,
        r, nw, win, cw, cb, wx, wdt, db, al, ds, wout, cs, ss,
        hx, own, rup, rdn, uf, xi, xc, dt, dx, sv, bc, pown, pin, yall, acc, s1o, s1i, s2o, s2i, s3o, s3i, sto, sti,
        ld_sem, win_sem, out_sem, ssm_sem, up_s, up_r, dn_s, dn_r, p_s, p_r, ag_s, ag_r, s_s, s_r, st_s, st_r,
    ):
        dp, me, ty = lax.axis_index("dp"), lax.axis_index("tx"), lax.axis_index("ty")
        core = lax.rem(ty, 2)
        barrier = pltpu.get_barrier_semaphore()
        tx_of = lambda k: (dp, k, ty)
        ty_of = lambda k: (dp, me, k)

        loads = {}
        names = dict(r=(r_hbm, r), nw=(nw_hbm, nw), cw=(cw_hbm, cw), cb=(cb_hbm, cb), db=(db_hbm, db), al=(al_hbm, al), ds=(ds_hbm, ds), cs=(cs_hbm, cs))
        for k, key in enumerate(names):
            loads[key] = pltpu.make_async_copy(names[key][0], names[key][1], ld_sem.at[k])
        for l in range(n_layer):
            for k, (key, src, dst) in enumerate((("wx", wx_hbm, wx), ("wdt", wdt_hbm, wdt), ("wout", wout_hbm, wout), ("ss", ss_hbm, ss))):
                loads[key, l] = pltpu.make_async_copy(src.at[l], dst.at[l], ld_sem.at[len(names) + 4 * l + k])
            for t in range(n_w):
                loads["win", l, t] = pltpu.make_async_copy(win_hbm.at[l, :, :, pl.ds(t * 128, 128)], win.at[l, t], win_sem.at[l, t])

        def start(*keys):
            for key in keys:
                loads[key].start()

        def wait(*keys):
            for key in keys:
                loads[key].wait()

        start("r", "nw")
        start(*[("win", 0, t) for t in range(n_w)])
        for k in range(1, n_tx):
            pl.semaphore_signal(barrier, 1, device_id=tx_of(lax.rem(me + k, n_tx)), device_id_type=MESH)
        for k in range(1, n_ty):
            pl.semaphore_signal(barrier, 1, device_id=ty_of(lax.rem(ty + k, n_ty)), device_id_type=MESH)
        start("cw", "cb", "db", "al", "ds", "cs", ("wx", 0))

        def remote(src, dst, ssem, rsem, dev):
            return pltpu.make_async_remote_copy(src_ref=src, dst_ref=dst, send_sem=ssem, recv_sem=rsem, device_id=dev, device_id_type=MESH)

        def up_copy(l, c, b):
            return remote(own.at[l, c, b], rup.at[l, c, b], up_s.at[l, c, b], up_r.at[l, c, b], tx_of(jnp.minimum(me + 1, last)))

        def dn_copy(l, c, b):
            return remote(own.at[l, c, b], rdn.at[l, c, b], dn_s.at[l, c, b], dn_r.at[l, c, b], tx_of(jnp.maximum(me - 1, 0)))

        def forward(l, c):
            for j in range(last, 0, -1):
                @pl.when(me + j <= last)
                def _():
                    b = me + j
                    @pl.when(me > 0)
                    def _():
                        up_copy(l, c, b).wait_recv()
                        own[l, c, b] = (own[l, c, b].astype(F32) + rup[l, c, b].astype(F32)).astype(BF16)
                    up_copy(l, c, b).start()

                @pl.when(me - j >= 0)
                def _():
                    b = me - j
                    @pl.when(me < last)
                    def _():
                        dn_copy(l, c, b).wait_recv()
                        own[l, c, b] = (own[l, c, b].astype(F32) + rdn[l, c, b].astype(F32)).astype(BF16)
                    dn_copy(l, c, b).start()

        def forward_end(l, c):
            for j in range(last, 0, -1):
                @pl.when(me + j <= last)
                def _():
                    up_copy(l, c, me + j).wait_send()

                @pl.when(me - j >= 0)
                def _():
                    dn_copy(l, c, me - j).wait_send()

        def finish(l, c):
            uf[...] = own[l, c, me].astype(F32)

            @pl.when(me > 0)
            def _():
                up_copy(l, c, me).wait_recv()
                uf[...] += rup[l, c, me].astype(F32)

            @pl.when(me < last)
            def _():
                dn_copy(l, c, me).wait_recv()
                uf[...] += rdn[l, c, me].astype(F32)
            return uf[...].astype(BF16)

        def stat_copy(l, k):
            return remote(sto.at[l], sti.at[l, me], st_s.at[l, k], st_r.at[l, me], tx_of(k))

        def stat_recv(l, k):
            return remote(sto.at[l], sti.at[l, k], st_s.at[l, k], st_r.at[l, k], tx_of(k))

        def p_copy(l, k):
            return remote(pown.at[l], pin.at[l, ty], p_s.at[l, k], p_r.at[l, ty], ty_of(k))

        def p_recv(l, k):
            return remote(pown.at[l], pin.at[l, k], p_s.at[l, k], p_r.at[l, k], ty_of(k))

        def ag_up(l, c, b):
            return remote(yall.at[l, c, b], yall.at[l, c, b], ag_s.at[l, c, 0, b], ag_r.at[l, c, b], tx_of(jnp.minimum(me + 1, last)))

        def ag_dn(l, c, b):
            return remote(yall.at[l, c, b], yall.at[l, c, b], ag_s.at[l, c, 1, b], ag_r.at[l, c, b], tx_of(jnp.maximum(me - 1, 0)))

        def gather_start(l, c):
            @pl.when(me < last)
            def _():
                ag_up(l, c, me).start()

            @pl.when(me > 0)
            def _():
                ag_dn(l, c, me).start()

        def gather_pass(l, c):
            for j in range(1, n_tx):
                @pl.when(me - j >= 0)
                def _():
                    ag_up(l, c, me - j).wait_recv()
                    @pl.when(me < last)
                    def _():
                        ag_up(l, c, me - j).start()

                @pl.when(me + j <= last)
                def _():
                    ag_dn(l, c, me + j).wait_recv()
                    @pl.when(me > 0)
                    def _():
                        ag_dn(l, c, me + j).start()

        def gather_end(l, c):
            for j in range(0, n_tx):
                @pl.when(jnp.logical_and(me - j >= 0, me < last))
                def _():
                    ag_up(l, c, me - j).wait_send()

                @pl.when(jnp.logical_and(me + j <= last, me > 0))
                def _():
                    ag_dn(l, c, me + j).wait_send()

        partner = ty_of(ty + 1 - 2 * core)
        across = ty_of(lax.rem(ty + 2, n_ty))
        mine = pl.ds(pl.multiple_of(core * half, half), half)
        other = pl.ds(pl.multiple_of((1 - core) * half, half), half)

        def s1_copy(l, q):
            return remote(s1o.at[l, q], s1i.at[l, q], s_s.at[l, 0, q], s_r.at[l, 0, q], partner)

        def s2_copy(l, q):
            return remote(s2o.at[l, q], s2i.at[l, q], s_s.at[l, 1, q], s_r.at[l, 1, q], across)

        def s3_copy(l, q):
            return remote(s3o.at[l, q], s3i.at[l, q], s_s.at[l, 2, q], s_r.at[l, 2, q], partner)

        row_i = lax.broadcasted_iota(jnp.int32, (128, 256), 0)
        col_i = lax.broadcasted_iota(jnp.int32, (128, 256), 1)
        pick = [(col_i == 2 * row_i + k).astype(F32).astype(BF16) for k in range(2)]

        outs = []

        def put(src, dst, sem):
            cp = pltpu.make_async_copy(src, dst, sem)
            cp.start()
            outs.append(cp)

        for l in range(n_layer):
            if l == 0:
                wait("r", "nw")
            sq = jnp.sum(r[...] * r[...], axis=-1, keepdims=True)
            sto[l] = jnp.broadcast_to(sq, (rows, 128)).T[0:8, :]
            if l == 0:
                pl.semaphore_wait(barrier, n_tx + n_ty - 2)
            for j in range(1, n_tx):
                stat_copy(l, lax.rem(me + j, n_tx)).start()
            sti[l, me] = sto[l]
            for j in range(1, n_tx):
                stat_recv(l, lax.rem(me + j, n_tx)).wait_recv()
            tot = sti[l, 0]
            for k in range(1, n_tx):
                tot = tot + sti[l, k]
            scale = lax.rsqrt(jnp.broadcast_to(tot[0:1, :], (128, rows)).T / d_model + NORM_EPS)
            for j in range(d_loc // 128):
                cols = pl.ds(j * 128, 128)
                h = (r[:, cols] * scale * nw[l : l + 1, cols]).astype(BF16)
                for k in range(2):
                    hx[k, :, pl.ds(j * 256, 256)] = dot(h, pick[k]).astype(BF16)

            def project(c):
                k, cc = c // n_c, c % n_c
                for t in range(0, chunk // 128, 2):
                    tile = cc * (chunk // 128) + t
                    if k == 0:
                        wait(("win", l, tile), ("win", l, tile + 1))
                    w = jnp.concatenate([win.at[l, tile + i].reshape(2 * d_loc, 128)[...] for i in range(2)], axis=1)
                    part = dot(hx[k], w).astype(BF16)
                    for b in range(n_tx):
                        own[l, c, b, :, pl.ds(t * 128, 256)] = part[b * blk : (b + 1) * blk, :]

            project(0)
            for c in range(1, n_c + 2):
                project(c)
                forward(l, c - 1)
            if l == 0:
                start(("wdt", 0), ("ss", 0), ("wout", 0))
                wait("cw", "cb", "db", "al", "ds", "cs")
            wait(("wx", l))
            p_part = jnp.zeros((blk, rank + 2 * n_state), F32)
            for c in range(n_c):
                cols = pl.ds(c * chunk, chunk)
                x_new = finish(l, c)
                xi[l, :, cols] = x_new
                val = x_new.astype(F32) * cw[l, 3:4, cols] + cb[l : l + 1, cols]
                for k in range(3):
                    val = val + cs[l, k, :, cols].astype(F32) * cw[l, k : k + 1, cols]
                x_act = (val * jax.nn.sigmoid(val)).astype(BF16)
                xc[:, cols] = x_act.astype(F32)
                p_part = p_part + lax.dot_general(x_act, wx[l, :, cols], (((1,), (1,)), ((), ())), preferred_element_type=F32)
            put(xi.at[l], conv_out.at[l, 2], out_sem.at[l, 0])
            put(cs.at[l, pl.ds(1, 2)], conv_out.at[l, pl.ds(0, 2)], out_sem.at[l, 1])
            pown[l] = p_part.astype(BF16)
            for j in range(1, n_ty):
                p_copy(l, lax.rem(ty + j, n_ty)).start()
            for c in range(n_c + 2, 2 * n_c):
                project(c)
                forward(l, c - 1)
            if l + 1 < n_layer:
                start(*[("win", l + 1, t) for t in range(n_w)])
                start(("wx", l + 1), ("wdt", l + 1), ("ss", l + 1), ("wout", l + 1))
            for j in range(1, n_ty):
                k = lax.rem(ty + j, n_ty)
                p_recv(l, k).wait_recv()
                p_part = p_part + pin[l, k].astype(F32)
            dt_low = p_part[:, :rank]
            dt_low = (dt_low * lax.rsqrt(jnp.mean(dt_low * dt_low, axis=-1, keepdims=True) + INNER_EPS)).astype(BF16)
            b_mat = p_part[:, rank : rank + n_state]
            b_mat = b_mat * lax.rsqrt(jnp.mean(b_mat * b_mat, axis=-1, keepdims=True) + INNER_EPS)
            c_mat = p_part[:, rank + n_state :]
            c_mat = c_mat * lax.rsqrt(jnp.mean(c_mat * c_mat, axis=-1, keepdims=True) + INNER_EPS)
            for i in range(2):
                mat_t = (b_mat, c_mat)[i].T
                for b in range(blk):
                    bc[i, b] = jnp.broadcast_to(mat_t[:, b : b + 1], (n_state, 128))
            forward(l, 2 * n_c - 1)
            wait(("wdt", l), ("ss", l))
            for c in range(n_c):
                cols = pl.ds(c * chunk, chunk)
                raw = dot(dt_low, wdt[l, :, cols]) + db[l : l + 1, cols]
                delta = jnp.maximum(raw, 0.0) + jnp.log1p(jnp.exp(-jnp.abs(raw)))
                dt[:, cols] = delta
                dx[:, cols] = delta * xc[:, cols]
                neg_a = -jnp.exp(al[l, :, cols]) * LOG2E

                def row_step(b, carry):
                    row = pl.ds(b, 1)
                    b_row = jnp.concatenate([bc[0, b]] * (chunk // 128), axis=1)
                    c_row = jnp.concatenate([bc[1, b]] * (chunk // 128), axis=1)
                    s_new = jnp.exp2(dt[row, cols] * neg_a) * ss[l, b, :, cols] + dx[row, cols] * b_row
                    ss[l, b, :, cols] = s_new
                    sv[row, cols] = jnp.sum(s_new * c_row, axis=0, keepdims=True)
                    return carry

                lax.fori_loop(0, blk, row_step, 0, unroll=4)
                put(ss.at[l, :, :, cols], ssm_out.at[l, :, :, cols], ssm_sem.at[l, c])
                z_new = finish(l, n_c + c).astype(F32)
                y = (sv[:, cols] + ds[l : l + 1, cols] * xc[:, cols]) * (z_new * jax.nn.sigmoid(z_new))
                yall[l, c, me] = y.astype(BF16)
                gather_start(l, c)
                if c > 0:
                    gather_pass(l, c - 1)
            wait(("wout", l))
            for c in range(n_c):
                if c == n_c - 1:
                    gather_pass(l, c)
                y_all = yall[l, c].reshape(rows, chunk)
                for q in range(n_q):
                    qc = pl.ds(q * qw, qw)
                    out = dot(y_all, wout[l, pl.ds(c * chunk, chunk), qc])
                    acc[:, qc] = out if c == 0 else acc[:, qc] + out
                    if c == n_c - 1:
                        s1o[l, q] = acc[other, qc].astype(BF16)
                        s1_copy(l, q).start()
            for q in range(n_q):
                s1_copy(l, q).wait_recv()
                s2o[l, q] = (acc[mine, pl.ds(q * qw, qw)] + s1i[l, q].astype(F32)).astype(BF16)
                s2_copy(l, q).start()
            for q in range(n_q):
                qc = pl.ds(q * qw, qw)
                s2_copy(l, q).wait_recv()
                tot = (s2o[l, q].astype(F32) + s2i[l, q].astype(F32)).astype(BF16)
                s3o[l, q] = tot
                s3_copy(l, q).start()
                r[mine, qc] += tot.astype(F32)
            for q in range(n_q):
                s3_copy(l, q).wait_recv()
                r[other, pl.ds(q * qw, qw)] += s3i[l, q].astype(F32)

        put(r, r_out, out_sem.at[0, 2])
        for l in range(n_layer):
            for c in range(2 * n_c):
                forward_end(l, c)
            for j in range(1, n_tx):
                stat_copy(l, lax.rem(me + j, n_tx)).wait_send()
            for j in range(1, n_ty):
                p_copy(l, lax.rem(ty + j, n_ty)).wait_send()
            for c in range(n_c):
                gather_end(l, c)
            for q in range(n_q):
                s1_copy(l, q).wait_send()
                s2_copy(l, q).wait_send()
                s3_copy(l, q).wait_send()
        for cp in outs:
            cp.wait()

    dma = lambda *s: pltpu.SemaphoreType.DMA(s)
    vm = lambda t, *s: pltpu.VMEM(s, t)
    nl = n_layer
    p_w = rank + 2 * n_state
    scratch = [
        vm(F32, rows, d_loc), vm(F32, nl, d_loc), vm(BF16, nl, n_w, d_loc, 2, 128), vm(F32, nl, 4, chan), vm(F32, nl, chan),
        vm(BF16, nl, p_w, chan), vm(BF16, nl, rank, chan), vm(F32, nl, chan), vm(F32, nl, n_state, chan), vm(F32, nl, chan),
        vm(BF16, nl, chan, d_loc), vm(BF16, nl, 3, blk, chan), vm(F32, nl, blk, n_state, chan),
        vm(BF16, 2, rows, 2 * d_loc), vm(BF16, nl, 2 * n_c, n_tx, blk, chunk), vm(BF16, nl, 2 * n_c, n_tx, blk, chunk), vm(BF16, nl, 2 * n_c, n_tx, blk, chunk),
        vm(F32, blk, chunk), vm(BF16, nl, blk, chan), vm(F32, blk, chan), vm(F32, blk, chan), vm(F32, blk, chan), vm(F32, blk, chan),
        vm(F32, 2, blk, n_state, 128), vm(BF16, nl, blk, p_w), vm(BF16, nl, n_ty, blk, p_w),
        vm(BF16, nl, n_c, n_tx, blk, chunk), vm(F32, rows, d_loc),
        *[vm(BF16, nl, n_q, half, qw) for _ in range(6)],
        vm(F32, nl, 8, 128), vm(F32, nl, n_tx, 8, 128),
        dma(8 + 4 * nl), dma(nl, n_w), dma(nl, 3), dma(nl, n_c),
        *[dma(nl, 2 * n_c, n_tx) for _ in range(4)],
        dma(nl, n_ty), dma(nl, n_ty), dma(nl, n_c, 2, n_tx), dma(nl, n_c, n_tx), dma(nl, 3, n_q), dma(nl, 3, n_q),
        dma(nl, n_tx), dma(nl, n_tx),
    ]
    return kernel, scratch


def solution(mesh):
    n_tx, n_ty = mesh.shape["tx"], mesh.shape["ty"]

    def local_step(residual, norm_w, w_in, conv_w, conv_b, w_x, w_dt, dt_bias, a_log, d_skip, w_out, conv_state, ssm_state):
        rows, d_loc = residual.shape
        n_layer, _, _, chan = w_in.shape
        rank, n_state = w_dt.shape[1], a_log.shape[-1]
        blk = rows // n_tx
        kernel, scratch = make_kernel(n_layer, n_tx, n_ty, rows, d_loc, chan, rank, n_state, 512)
        r_out, conv_out, ssm_out = pl.pallas_call(
            kernel,
            out_shape=(
                jax.ShapeDtypeStruct((rows, d_loc), F32),
                jax.ShapeDtypeStruct((n_layer, 3, blk, chan), BF16),
                jax.ShapeDtypeStruct((n_layer, blk, n_state, chan), F32),
            ),
            in_specs=[ANY] * 13,
            out_specs=(ANY, ANY, ANY),
            scratch_shapes=scratch,
            compiler_params=pltpu.CompilerParams(collective_id=0, has_side_effects=True, vmem_limit_bytes=67043328),
            name="mixer",
        )(
            residual, norm_w, w_in, conv_w.transpose(0, 2, 1), conv_b, w_x.transpose(0, 2, 1), w_dt, dt_bias,
            a_log.transpose(0, 2, 1), d_skip, w_out, conv_state.transpose(0, 3, 1, 2), ssm_state.transpose(0, 1, 3, 2),
        )
        return r_out, conv_out.transpose(0, 2, 3, 1), ssm_out.transpose(0, 1, 3, 2)

    cache_spec = P(None, ("dp", "tx"), "ty", None)
    in_specs = (P("dp", "tx"), P(None, "tx"), P(None, "tx", None, "ty"), P(None, "ty", None), P(None, "ty"), P(None, "ty", None), P(None, None, "ty"), P(None, "ty"), P(None, "ty", None), P(None, "ty"), P(None, "ty", "tx"), cache_spec, cache_spec)
    out_specs = (P("dp", "tx"), cache_spec, cache_spec)
    return jax.shard_map(local_step, mesh=mesh, in_specs=in_specs, out_specs=out_specs, check_vma=False)
```

```python
import jax
import jax.numpy as jnp
from jax import lax
from jax.experimental import pallas as pl
from jax.experimental.pallas import tpu as pltpu
from jax.sharding import PartitionSpec as P

NORM_EPS = 1e-5
INNER_EPS = 1e-6
LOG2E = 1.4426950408889634
BF16, F32 = jnp.bfloat16, jnp.float32
MESH = pl.DeviceIdType.MESH
ANY = pl.BlockSpec(memory_space=pl.ANY)
VMEM = pl.BlockSpec(memory_space=pltpu.VMEM)


def dot(a, b):
    return jnp.dot(a, b, preferred_element_type=F32)


def make_kernel(n_layer, n_tx, n_ty, rows, d_loc, chan, rank, n_state, chunk, n_g, n_q):
    blk = rows // n_tx
    hb = blk // n_g
    rg = n_tx * hb
    half = rg // 2
    n_c = chan // chunk
    d_model = d_loc * n_tx
    qw = d_loc // n_q
    n_w = chan // 128

    def kernel(
        r_hbm, nw_hbm, win_hbm, cw_hbm, cb_hbm, wx_hbm, wdt_hbm, db_hbm, al_hbm, ds_hbm, wout_hbm, cs_hbm, ss_hbm,
        r, xi, cs, ss,
        nw, win, cw, cb, wx, wdt, db, al, ds, wout,
        hx, own, cmb, fin, xc, dt, dx, sv, bc, pown, pin, yall, acc, s1o, s1i, s2o, s2i, s3o, s3i, sto, sti,
        ld_sem, r_sem, win_sem, rs_s, cm_r, fn_r, p_s, p_r, ag_s, ag_r, s_s, s_r, st_s, st_r,
    ):
        dp, me, ty = lax.axis_index("dp"), lax.axis_index("tx"), lax.axis_index("ty")
        core = lax.rem(ty, 2)
        mate = me + 1 - 2 * lax.rem(me, 2)
        mid = (me * (3 - me)) // 2
        o_end = 3 - me + mid * (me - mate)
        o_mid = 3 - mate + mid * (mate - me)
        barrier = pltpu.get_barrier_semaphore()

        def tx_of(k):
            return (dp, k, ty)

        def ty_of(k):
            return (dp, me, k)

        def remote(src, dst, ssem, rsem, dev):
            return pltpu.make_async_remote_copy(src_ref=src, dst_ref=dst, send_sem=ssem, recv_sem=rsem, device_id=dev, device_id_type=MESH)

        loads = {}
        for g in range(n_g):
            for b in range(n_tx):
                loads["r", g, b] = pltpu.make_async_copy(r_hbm.at[pl.ds(b * blk + g * hb, hb)], r.at[g, pl.ds(b * hb, hb)], r_sem.at[g, b])
        names = dict(nw=(nw_hbm, nw), cw=(cw_hbm, cw), cb=(cb_hbm, cb), db=(db_hbm, db), al=(al_hbm, al), ds=(ds_hbm, ds), cs=(cs_hbm, cs))
        for k, key in enumerate(names):
            loads[key] = pltpu.make_async_copy(names[key][0], names[key][1], ld_sem.at[k])
        for l in range(n_layer):
            for k, (key, src, dst) in enumerate((("wx", wx_hbm, wx), ("wdt", wdt_hbm, wdt), ("wout", wout_hbm, wout), ("ss", ss_hbm, ss))):
                loads[key, l] = pltpu.make_async_copy(src.at[l], dst.at[l], ld_sem.at[len(names) + 4 * l + k])
            for t in range(n_w):
                loads["win", l, t] = pltpu.make_async_copy(win_hbm.at[l, :, :, pl.ds(t * 128, 128)], win.at[l, t], win_sem.at[l, t])

        def start(*keys):
            for key in keys:
                loads[key].start()

        def wait(*keys):
            for key in keys:
                loads[key].wait()

        def stat_copy(l, g, k):
            return remote(sto.at[l, g], sti.at[l, g, me], st_s.at[l, g, k], st_r.at[l, g, me], tx_of(k))

        def stat_recv(l, g, k):
            return remote(sto.at[l, g], sti.at[l, g, k], st_s.at[l, g, k], st_r.at[l, g, k], tx_of(k))

        def to_mate(l, g, c):
            return remote(own.at[l, g, c, mate], fin.at[l, g, c, 0], rs_s.at[l, g, c, 2], fn_r.at[l, g, c, 0], tx_of(mate))

        def to_mid(l, g, c, k):
            return remote(own.at[l, g, c, (o_end, o_mid)[k]], cmb.at[l, g, c, k], rs_s.at[l, g, c, k], cm_r.at[l, g, c, k], tx_of(mate))

        def to_far(l, g, c, k):
            b = (o_end, o_mid)[k]
            return remote(own.at[l, g, c, b], fin.at[l, g, c, 1], rs_s.at[l, g, c, k], fn_r.at[l, g, c, 1], tx_of(b))

        def p_copy(l, g, k):
            return remote(pown.at[l, g], pin.at[l, g, ty], p_s.at[l, g, k], p_r.at[l, g, ty], ty_of(k))

        def p_recv(l, g, k):
            return remote(pown.at[l, g], pin.at[l, g, k], p_s.at[l, g, k], p_r.at[l, g, k], ty_of(k))

        def ag_copy(l, g, c, b, k, dev):
            return remote(yall.at[l, g, c, b], yall.at[l, g, c, b], ag_s.at[l, g, c, k], ag_r.at[l, g, c, b], tx_of(dev))

        partner = ty_of(ty + 1 - 2 * core)
        across = ty_of(lax.rem(ty + 2, n_ty))
        mine = pl.ds(pl.multiple_of(core * half, half), half)
        other = pl.ds(pl.multiple_of((1 - core) * half, half), half)

        def s_copy(i, l, g, q):
            src, dst = ((s1o, s1i), (s2o, s2i), (s3o, s3i))[i]
            return remote(src.at[l, g, q], dst.at[l, g, q], s_s.at[l, g, i, q], s_r.at[l, g, i, q], across if i == 1 else partner)

        def stat(l, g):
            sq = jnp.sum(r[g] * r[g], axis=-1, keepdims=True)
            sto[l, g] = jnp.broadcast_to(sq, (rg, 128)).T[0:8, :]

        def stat_send(l, g):
            for j in range(1, n_tx):
                stat_copy(l, g, lax.rem(me + j, n_tx)).start()
            sti[l, g, me] = sto[l, g]

        def head(l, g):
            for j in range(1, n_tx):
                stat_recv(l, g, lax.rem(me + j, n_tx)).wait_recv()
            tot = sti[l, g, 0]
            for k in range(1, n_tx):
                tot = tot + sti[l, g, k]
            scale = lax.rsqrt(jnp.broadcast_to(tot[0:1, :], (128, rg)).T / d_model + NORM_EPS)
            row_i = lax.broadcasted_iota(jnp.int32, (128, 256), 0)
            col_i = lax.broadcasted_iota(jnp.int32, (128, 256), 1)
            pick = [(col_i == 2 * row_i + k).astype(F32).astype(BF16) for k in range(2)]
            for j in range(d_loc // 128):
                cols = pl.ds(j * 128, 128)
                h = (r[g, :, cols] * scale * nw[l : l + 1, cols]).astype(BF16)
                for k in range(2):
                    hx[g, k * rg : (k + 1) * rg, pl.ds(j * 256, 256)] = dot(h, pick[k]).astype(BF16)

        def project(l, gs, c):
            lhs = hx[gs[0]] if len(gs) == 1 else hx[...].reshape(n_g * 2 * rg, 2 * d_loc)
            for t in range(0, chunk // 128, 2):
                tile = c * (chunk // 128) + t
                if gs[0] == 0:
                    wait(("win", l, tile), ("win", l, tile + 1))
                w = jnp.concatenate([win.at[l, tile + i].reshape(2 * d_loc, 128)[...] for i in range(2)], axis=1)
                part = dot(lhs, w).astype(BF16)
                for i, g in enumerate(gs):
                    for k in range(2):
                        for b in range(n_tx):
                            at = (2 * i + k) * rg + b * hb
                            own[l, g, k * n_c + c, b, :, pl.ds(t * 128, 256)] = part[at : at + hb, :]

        def send(l, g, c):
            @pl.when(mid == 0)
            def _():
                to_mid(l, g, c, 0).start()
                to_mid(l, g, c, 1).start()
            to_mate(l, g, c).start()

        def send_z(l, g):
            for c in range(n_c, 2 * n_c):
                send(l, g, c)

        def combine(l, g, c):
            @pl.when(mid == 1)
            def _():
                for k in range(2):
                    b = (o_end, o_mid)[k]
                    to_mid(l, g, c, k).wait_recv()
                    own[l, g, c, b] = (own[l, g, c, b].astype(F32) + cmb[l, g, c, k].astype(F32)).astype(BF16)
                    to_far(l, g, c, k).start()

        def finish(l, g, c):
            to_mate(l, g, c).wait_recv()
            to_far(l, g, c, 0).wait_recv()
            return (own[l, g, c, me].astype(F32) + fin[l, g, c, 0].astype(F32) + fin[l, g, c, 1].astype(F32)).astype(BF16)

        def x_phase(l, g):
            hrow = pl.ds(g * hb, hb)
            p_part = jnp.zeros((hb, rank + 2 * n_state), F32)
            for c in range(n_c):
                cols = pl.ds(c * chunk, chunk)
                x_new = finish(l, g, c)
                xi[l, hrow, cols] = x_new
                val = x_new.astype(F32) * cw[l, 3:4, cols] + cb[l : l + 1, cols]
                for k in range(3):
                    val = val + cs[l, k, hrow, cols].astype(F32) * cw[l, k : k + 1, cols]
                x_act = (val * jax.nn.sigmoid(val)).astype(BF16)
                xc[g, :, cols] = x_act.astype(F32)
                p_part = p_part + lax.dot_general(x_act, wx[l, :, cols], (((1,), (1,)), ((), ())), preferred_element_type=F32)
            pown[l, g] = p_part.astype(BF16)
            for j in range(1, n_ty):
                p_copy(l, g, lax.rem(ty + j, n_ty)).start()

        def d_phase(l, g):
            p_sum = pown[l, g].astype(F32)
            for j in range(1, n_ty):
                k = lax.rem(ty + j, n_ty)
                p_recv(l, g, k).wait_recv()
                p_sum = p_sum + pin[l, g, k].astype(F32)
            dt_low = p_sum[:, :rank]
            dt_low = (dt_low * lax.rsqrt(jnp.mean(dt_low * dt_low, axis=-1, keepdims=True) + INNER_EPS)).astype(BF16)
            for i in range(2):
                mat = p_sum[:, rank + i * n_state : rank + (i + 1) * n_state]
                mat_t = (mat * lax.rsqrt(jnp.mean(mat * mat, axis=-1, keepdims=True) + INNER_EPS)).T
                for b in range(hb):
                    bc[i, b] = jnp.broadcast_to(mat_t[:, b : b + 1], (n_state, 128))
            for c in range(n_c):
                cols = pl.ds(c * chunk, chunk)
                raw = dot(dt_low, wdt[l, :, cols]) + db[l : l + 1, cols]
                delta = jnp.maximum(raw, 0.0) + jnp.log1p(jnp.exp(-jnp.abs(raw)))
                dt[:, cols] = delta
                dx[:, cols] = delta * xc[g, :, cols]
                neg_a = -jnp.exp(al[l, :, cols]) * LOG2E

                def row_step(b, carry):
                    row = pl.ds(b, 1)
                    b_row = jnp.concatenate([bc[0, b]] * (chunk // 128), axis=1)
                    c_row = jnp.concatenate([bc[1, b]] * (chunk // 128), axis=1)
                    at = g * hb + b
                    s_new = jnp.exp2(dt[row, cols] * neg_a) * ss[l, at, :, cols] + dx[row, cols] * b_row
                    ss[l, at, :, cols] = s_new
                    sv[g, row, cols] = jnp.sum(s_new * c_row, axis=0, keepdims=True)
                    return carry

                lax.fori_loop(0, hb, row_step, 0, unroll=4)

        def y_phase(l, g, c):
            cols = pl.ds(c * chunk, chunk)
            z_new = finish(l, g, n_c + c).astype(F32)
            y = (sv[g, :, cols] + ds[l : l + 1, cols] * xc[g, :, cols]) * (z_new * jax.nn.sigmoid(z_new))
            yall[l, g, c, me] = y.astype(BF16)
            ag_copy(l, g, c, me, 0, mate).start()

            @pl.when(mid == 1)
            def _():
                ag_copy(l, g, c, me, 1, 3 - me).start()

        def gather_1(l, g, c):
            ag_copy(l, g, c, mate, 0, mate).wait_recv()

            @pl.when(mid == 1)
            def _():
                ag_copy(l, g, c, mate, 2, 3 - me).start()

        def gather_2(l, g, c):
            ag_copy(l, g, c, o_mid, 0, mate).wait_recv()

            @pl.when(mid == 1)
            def _():
                ag_copy(l, g, c, o_mid, 3, mate).start()

            ag_copy(l, g, c, o_end, 0, mate).wait_recv()

            @pl.when(mid == 1)
            def _():
                ag_copy(l, g, c, o_end, 4, mate).start()

        def w_phase(l, g, c):
            y_all = yall[l, g, c].reshape(rg, chunk)
            for q in range(n_q):
                qc = pl.ds(q * qw, qw)
                out = dot(y_all, wout[l, pl.ds(c * chunk, chunk), qc])
                acc[g, :, qc] = out if c == 0 else acc[g, :, qc] + out
                if c == n_c - 1:
                    s1o[l, g, q] = acc[g, other, qc].astype(BF16)
                    s_copy(0, l, g, q).start()

        def sum_1(l, g):
            for q in range(n_q):
                s_copy(0, l, g, q).wait_recv()
                s2o[l, g, q] = (acc[g, mine, pl.ds(q * qw, qw)] + s1i[l, g, q].astype(F32)).astype(BF16)
                s_copy(1, l, g, q).start()

        def sum_2(l, g):
            for q in range(n_q):
                qc = pl.ds(q * qw, qw)
                s_copy(1, l, g, q).wait_recv()
                tot = (s2o[l, g, q].astype(F32) + s2i[l, g, q].astype(F32)).astype(BF16)
                s3o[l, g, q] = tot
                s_copy(2, l, g, q).start()
                r[g, mine, qc] += tot.astype(F32)

        def sum_3(l, g):
            for q in range(n_q):
                s_copy(2, l, g, q).wait_recv()
                r[g, other, pl.ds(q * qw, qw)] += s3i[l, g, q].astype(F32)

        ph = dict(
            stat=stat, stat_send=stat_send, head=head, send=send, send_z=send_z, combine=combine, x=x_phase, d=d_phase,
            y=y_phase, g1=gather_1, g2=gather_2, w=w_phase, s1=sum_1, s2=sum_2, s3=sum_3,
        )

        def run(name, *args):
            with jax.named_scope(name + "_" + "_".join(map(str, args))):
                ph[name](*args)

        def proj(l, gs, c):
            with jax.named_scope(f"proj_{l}_{gs[0]}_{c}"):
                project(l, gs, c)
            for g in gs:
                send(l, g, c)

        groups = range(n_g)
        for g in groups:
            start(*[("r", g, b) for b in range(n_tx)])
        start("nw", *[("win", 0, t) for t in range(n_w)])
        for k in range(1, n_tx):
            pl.semaphore_signal(barrier, 1, device_id=tx_of(lax.rem(me + k, n_tx)), device_id_type=MESH)
        for k in range(1, n_ty):
            pl.semaphore_signal(barrier, 1, device_id=ty_of(lax.rem(ty + k, n_ty)), device_id_type=MESH)
        for g in groups:
            wait(*[("r", g, b) for b in range(n_tx)])
            run("stat", 0, g)
        pl.semaphore_wait(barrier, n_tx + n_ty - 2)
        for g in groups:
            run("stat_send", 0, g)
        start("cw", "cb", "db", "al", "ds", "cs", ("wx", 0), ("wdt", 0), ("ss", 0), ("wout", 0))
        wait("nw")
        for l in range(n_layer):
            if l == 0:
                for g in groups:
                    run("head", l, g)
                for c in range(n_c):
                    proj(l, (0, 1), c)
                    if c > 1:
                        run("combine", l, 0, c - 2)
                        run("combine", l, 1, c - 2)
                start(*[("win", 1, t) for t in range(n_w)])
                start(("wx", 1), ("wdt", 1), ("ss", 1), ("wout", 1))
                wait("cw", "cb", "db", "al", "ds", "cs", ("wx", 0))
                run("send_z", l, 0)
                run("send_z", l, 1)
                for c in (n_c - 2, n_c - 1):
                    run("combine", l, 0, c)
                for c in (n_c - 2, n_c - 1):
                    run("combine", l, 1, c)
            else:
                run("head", l, 0)
                proj(l, (0,), 0)
                proj(l, (0,), 1)
                run("s1", l - 1, 1)
                run("combine", l, 0, 0)
                proj(l, (0,), 2)
                run("combine", l, 0, 1)
                proj(l, (0,), 3)
                run("send_z", l, 0)
                run("s2", l - 1, 1)
                run("combine", l, 0, 2)
                run("s3", l - 1, 1)
                run("stat", l, 1)
                run("stat_send", l, 1)
                run("combine", l, 0, 3)
                wait(("wx", l))
            run("x", l, 0)
            if l > 0:
                run("head", l, 1)
                for c in range(n_c):
                    proj(l, (1,), c)
                    run("combine", l, 0, n_c + c)
                    if c > 1:
                        run("combine", l, 1, c - 2)
                run("send_z", l, 1)
            else:
                for c in range(n_c):
                    run("combine", l, 0, n_c + c)
            if l == 0:
                run("x", l, 1)
            wait(("wdt", l), ("ss", l))
            run("d", l, 0)
            for c in range(n_c):
                run("y", l, 0, c)
            if l > 0:
                run("combine", l, 1, n_c - 2)
                run("combine", l, 1, n_c - 1)
                for c in range(n_c):
                    run("g1", l, 0, c)
                run("x", l, 1)
            else:
                for c in range(n_c):
                    run("g1", l, 0, c)
            for c in range(n_c):
                run("combine", l, 1, n_c + c)
            wait(("wout", l))
            for c in range(n_c):
                run("g2", l, 0, c)
                run("w", l, 0, c)
            run("d", l, 1)
            run("s1", l, 0)
            for c in range(n_c):
                run("y", l, 1, c)
            run("s2", l, 0)
            run("s3", l, 0)
            if l + 1 < n_layer:
                run("stat", l + 1, 0)
                run("stat_send", l + 1, 0)
            for c in range(n_c):
                run("g1", l, 1, c)
            for c in range(n_c):
                run("g2", l, 1, c)
                run("w", l, 1, c)
        run("s1", n_layer - 1, 1)
        run("s2", n_layer - 1, 1)
        run("s3", n_layer - 1, 1)

        for l in range(n_layer):
            for g in groups:
                for j in range(1, n_tx):
                    stat_copy(l, g, lax.rem(me + j, n_tx)).wait_send()
                for c in range(2 * n_c):
                    to_mate(l, g, c).wait_send()
                    to_mid(l, g, c, 0).wait_send()
                    to_mid(l, g, c, 1).wait_send()
                for j in range(1, n_ty):
                    p_copy(l, g, lax.rem(ty + j, n_ty)).wait_send()
                for c in range(n_c):
                    ag_copy(l, g, c, me, 0, mate).wait_send()

                    @pl.when(mid == 1)
                    def _():
                        for k in range(1, 5):
                            ag_copy(l, g, c, me, k, mate).wait_send()
                for q in range(n_q):
                    for i in range(3):
                        s_copy(i, l, g, q).wait_send()

    def dma(*s):
        return pltpu.SemaphoreType.DMA(s)

    def vm(t, *s):
        return pltpu.VMEM(s, t)

    nl, p_w = n_layer, rank + 2 * n_state
    scratch = [
        vm(F32, nl, d_loc), vm(BF16, nl, n_w, d_loc, 2, 128), vm(F32, nl, 4, chan), vm(F32, nl, chan),
        vm(BF16, nl, p_w, chan), vm(BF16, nl, rank, chan), vm(F32, nl, chan), vm(F32, nl, n_state, chan), vm(F32, nl, chan),
        vm(BF16, nl, chan, d_loc),
        vm(BF16, n_g, 2 * rg, 2 * d_loc), vm(BF16, nl, n_g, 2 * n_c, n_tx, hb, chunk),
        vm(BF16, nl, n_g, 2 * n_c, 2, hb, chunk), vm(BF16, nl, n_g, 2 * n_c, 2, hb, chunk),
        vm(F32, n_g, hb, chan), vm(F32, hb, chan), vm(F32, hb, chan), vm(F32, n_g, hb, chan),
        vm(F32, 2, hb, n_state, 128), vm(BF16, nl, n_g, hb, p_w), vm(BF16, nl, n_g, n_ty, hb, p_w),
        vm(BF16, nl, n_g, n_c, n_tx, hb, chunk), vm(F32, n_g, rg, d_loc),
        *[vm(BF16, nl, n_g, n_q, half, qw) for _ in range(6)],
        vm(F32, nl, n_g, 8, rg), vm(F32, nl, n_g, n_tx, 8, rg),
        dma(7 + 4 * nl), dma(n_g, n_tx), dma(nl, n_w),
        dma(nl, n_g, 2 * n_c, 3), dma(nl, n_g, 2 * n_c, 2), dma(nl, n_g, 2 * n_c, 2),
        dma(nl, n_g, n_ty), dma(nl, n_g, n_ty), dma(nl, n_g, n_c, 5), dma(nl, n_g, n_c, n_tx),
        dma(nl, n_g, 3, n_q), dma(nl, n_g, 3, n_q), dma(nl, n_g, n_tx), dma(nl, n_g, n_tx),
    ]
    outs = (vm(F32, n_g, rg, d_loc), vm(BF16, nl, blk, chan), vm(BF16, nl, 3, blk, chan), vm(F32, nl, blk, n_state, chan))
    return kernel, outs, scratch


def store_kernel(r, xi, cs, ss, r_out, conv_out, ssm_out, sem):
    n_g, rg, _ = r.shape
    nl, blk = ss.shape[:2]
    hb = blk // n_g
    pairs = []
    for l in range(nl):
        for i in range(0, blk, 8):
            pairs.append((ss.at[l, pl.ds(i, 8)], ssm_out.at[l, pl.ds(i, 8)]))
    for l in range(nl):
        pairs.append((cs.at[l, pl.ds(1, 2)], conv_out.at[l, pl.ds(0, 2)]))
        pairs.append((xi.at[l], conv_out.at[l, 2]))
    for g in range(n_g):
        for b in range(rg // hb):
            pairs.append((r.at[g, pl.ds(b * hb, hb)], r_out.at[pl.ds(b * blk + g * hb, hb)]))
    copies = [pltpu.make_async_copy(src, dst, sem.at[i]) for i, (src, dst) in enumerate(pairs)]
    for cp in copies:
        cp.start()
    for cp in copies:
        cp.wait()


def solution(mesh):
    n_tx, n_ty = mesh.shape["tx"], mesh.shape["ty"]

    def local_step(residual, norm_w, w_in, conv_w, conv_b, w_x, w_dt, dt_bias, a_log, d_skip, w_out, conv_state, ssm_state):
        rows, d_loc = residual.shape
        n_layer, _, _, chan = w_in.shape
        rank, n_state = w_dt.shape[1], a_log.shape[-1]
        blk = rows // n_tx
        kernel, outs, scratch = make_kernel(n_layer, n_tx, n_ty, rows, d_loc, chan, rank, n_state, 512, 2, 2)
        parts = pl.pallas_call(
            kernel,
            out_shape=outs,
            in_specs=[ANY] * 13,
            out_specs=(VMEM,) * 4,
            scratch_shapes=scratch,
            compiler_params=pltpu.CompilerParams(collective_id=0, has_side_effects=True, vmem_limit_bytes=67043328 - 11 * 2**20),
            name="mixer",
        )(
            residual, norm_w, w_in, conv_w.transpose(0, 2, 1), conv_b, w_x.transpose(0, 2, 1), w_dt, dt_bias,
            a_log.transpose(0, 2, 1), d_skip, w_out, conv_state.transpose(0, 3, 1, 2), ssm_state.transpose(0, 1, 3, 2),
        )
        r_out, conv_out, ssm_out = pl.pallas_call(
            store_kernel,
            out_shape=(
                jax.ShapeDtypeStruct((rows, d_loc), F32),
                jax.ShapeDtypeStruct((n_layer, 3, blk, chan), BF16),
                jax.ShapeDtypeStruct((n_layer, blk, n_state, chan), F32),
            ),
            in_specs=[VMEM] * 4,
            out_specs=(ANY,) * 3,
            scratch_shapes=[pltpu.SemaphoreType.DMA((64,))],
            compiler_params=pltpu.CompilerParams(vmem_limit_bytes=12 * 2**20),
            name="store",
        )(*parts)
        return r_out, conv_out.transpose(0, 2, 3, 1), ssm_out.transpose(0, 1, 3, 2)

    cache_spec = P(None, ("dp", "tx"), "ty", None)
    in_specs = (P("dp", "tx"), P(None, "tx"), P(None, "tx", None, "ty"), P(None, "ty", None), P(None, "ty"), P(None, "ty", None), P(None, None, "ty"), P(None, "ty"), P(None, "ty", None), P(None, "ty"), P(None, "ty", "tx"), cache_spec, cache_spec)
    out_specs = (P("dp", "tx"), cache_spec, cache_spec)
    return jax.shard_map(local_step, mesh=mesh, in_specs=in_specs, out_specs=out_specs, check_vma=False)
```

```python
import jax
import jax.numpy as jnp
from jax import lax
from jax.experimental import pallas as pl
from jax.experimental.pallas import tpu as pltpu
from jax.sharding import PartitionSpec as P

NORM_EPS = 1e-5
INNER_EPS = 1e-6
LOG2E = 1.4426950408889634
BF16, F32 = jnp.bfloat16, jnp.float32
MESH = pl.DeviceIdType.MESH
ANY = pl.BlockSpec(memory_space=pl.ANY)
VMEM = pl.BlockSpec(memory_space=pltpu.VMEM)


def dot(a, b):
    return jnp.dot(a, b, preferred_element_type=F32)


def make_kernel(n_layer, n_tx, n_ty, rows, d_loc, chan, rank, n_state, chunk, n_g, n_q):
    blk = rows // n_tx
    hb = blk // n_g
    rg = n_tx * hb
    half = rg // 2
    n_c = chan // chunk
    d_model = d_loc * n_tx
    qw = d_loc // n_q
    n_w = chan // 128

    def kernel(
        r_hbm, nw_hbm, win_hbm, cw_hbm, cb_hbm, wx_hbm, wdt_hbm, db_hbm, al_hbm, ds_hbm, wout_hbm, cs_hbm, ss_hbm,
        r, xi, cs, ss,
        nw, win, cw, cb, wx, wdt, db, al, ds, wout,
        hx, own, cmb, fin, xc, dt, dx, sv, bc, pown, pin, yall, acc, so, si, sto, sti, sc,
        ld_sem, r_sem, win_sem, rs_s, cm_r, fn_r, p_s, p_r, ag_s, ag_r, s_s, s_r, st_s, st_r,
    ):
        dp, me, ty = lax.axis_index("dp"), lax.axis_index("tx"), lax.axis_index("ty")
        core = lax.rem(ty, 2)
        mate = me + 1 - 2 * lax.rem(me, 2)
        mid = (me * (3 - me)) // 2
        o_end = 3 - me + mid * (me - mate)
        o_mid = 3 - mate + mid * (mate - me)
        lo = 2 * (1 - me // 2)
        barrier = pltpu.get_barrier_semaphore()

        def tx_of(k):
            return (dp, k, ty)

        def ty_of(k):
            return (dp, me, k)

        def remote(src, dst, ssem, rsem, dev):
            return pltpu.make_async_remote_copy(src_ref=src, dst_ref=dst, send_sem=ssem, recv_sem=rsem, device_id=dev, device_id_type=MESH)

        loads = {}
        for g in range(n_g):
            for b in range(n_tx):
                loads["r", g, b] = pltpu.make_async_copy(r_hbm.at[pl.ds(b * blk + g * hb, hb)], r.at[g, pl.ds(b * hb, hb)], r_sem.at[g, b])
        names = dict(nw=(nw_hbm, nw), cw=(cw_hbm, cw), cb=(cb_hbm, cb), db=(db_hbm, db), al=(al_hbm, al), ds=(ds_hbm, ds), cs=(cs_hbm, cs))
        for k, key in enumerate(names):
            loads[key] = pltpu.make_async_copy(names[key][0], names[key][1], ld_sem.at[k])
        for l in range(n_layer):
            for k, (key, src, dst) in enumerate((("wx", wx_hbm, wx), ("wdt", wdt_hbm, wdt), ("wout", wout_hbm, wout), ("ss", ss_hbm, ss))):
                loads[key, l] = pltpu.make_async_copy(src.at[l], dst.at[l], ld_sem.at[len(names) + 4 * l + k])
            for t in range(n_w):
                loads["win", l, t] = pltpu.make_async_copy(win_hbm.at[l, :, :, pl.ds(t * 128, 128)], win.at[l, t], win_sem.at[l, t])

        def start(*keys):
            for key in keys:
                loads[key].start()

        def wait(*keys):
            for key in keys:
                loads[key].wait()

        partner_ty = ty + 1 - 2 * core
        partner = ty_of(partner_ty)
        across = ty_of(lax.rem(ty + 2, n_ty))
        mine = pl.ds(pl.multiple_of(core * half, half), half)
        other = pl.ds(pl.multiple_of((1 - core) * half, half), half)

        def stat_copy(l, g, j, rel):
            dev = (dp, lax.rem(me + j, n_tx), partner_ty if rel else ty)
            return remote(sto.at[l, g], sti.at[l, g, 2 * j + rel - 1], st_s, st_r.at[l, g], dev)

        def to_mate(l, g, c):
            return remote(own.at[l, g, c, mate], fin.at[l, g, c, 0], rs_s, fn_r.at[l, g, c], tx_of(mate))

        def to_mid(l, g, c):
            return remote(own.at[l, g, c, pl.ds(lo, 2)], cmb.at[l, g, c], rs_s, cm_r.at[l, g, c], tx_of(mate))

        def to_far(l, g, c, k):
            b = (o_end, o_mid)[k]
            return remote(own.at[l, g, c, b], fin.at[l, g, c, 1], rs_s, fn_r.at[l, g, c], tx_of(b))

        def p_copy(l, g, j):
            return remote(pown.at[l, g], pin.at[l, g, j - 1], p_s, p_r.at[l, g], ty_of(lax.rem(ty + j, n_ty)))

        def ag_copy(l, g, c, b, k, dev):
            return remote(yall.at[l, g, c, b], yall.at[l, g, c, b], ag_s, ag_r.at[l, g, c, k], tx_of(dev))

        def s_copy(i, l, g, q):
            return remote(so.at[i, l, g, q], si.at[i, l, g, q], s_s, s_r.at[l, g, i, q], across if i == 1 else partner)

        def all_of(ref, ssem, rsem):
            return remote(ref, ref, ssem, rsem, partner)

        def stat(l, g):
            part = r[g, mine, :]
            sq = jnp.sum(part * part, axis=-1, keepdims=True)
            sto[l, g] = jnp.broadcast_to(sq, (half, 128)).T[0:8, :]
            for j in range(n_tx - 1, -1, -1):
                for rel in range(2):
                    if j or rel:
                        stat_copy(l, g, j, rel).start()

        def head(l, g):
            all_of(sti.at[l, g], st_s, st_r.at[l, g]).wait_recv()
            for rel, at in enumerate((mine, other)):
                tot = sto[l, g] if rel == 0 else sti[l, g, 0]
                for j in range(1, n_tx):
                    tot = tot + sti[l, g, 2 * j + rel - 1]
                sc[at, :] = lax.rsqrt(jnp.broadcast_to(tot[0:1, :], (128, half)).T / d_model + NORM_EPS)
            scale = sc[...]
            row_i = lax.broadcasted_iota(jnp.int32, (128, 256), 0)
            col_i = lax.broadcasted_iota(jnp.int32, (128, 256), 1)
            pick = [(col_i == 2 * row_i + k).astype(F32).astype(BF16) for k in range(2)]
            for j in range(d_loc // 128):
                cols = pl.ds(j * 128, 128)
                h = (r[g, :, cols] * scale * nw[l : l + 1, cols]).astype(BF16)
                for k in range(2):
                    hx[g, k * rg : (k + 1) * rg, pl.ds(j * 256, 256)] = dot(h, pick[k]).astype(BF16)

        def project(l, gs, c):
            lhs = hx[gs[0]] if len(gs) == 1 else hx[...].reshape(n_g * 2 * rg, 2 * d_loc)
            for t in range(0, chunk // 128, 2):
                tile = c * (chunk // 128) + t
                if gs[0] == 0:
                    wait(("win", l, tile), ("win", l, tile + 1))
                w = jnp.concatenate([win.at[l, tile + i].reshape(2 * d_loc, 128)[...] for i in range(2)], axis=1)
                part = dot(lhs, w).astype(BF16)
                for i, g in enumerate(gs):
                    for k in range(2):
                        for b in range(n_tx):
                            at = (2 * i + k) * rg + b * hb
                            own[l, g, k * n_c + c, b, :, pl.ds(t * 128, 256)] = part[at : at + hb, :]

        def send(l, g, c):
            @pl.when(mid == 0)
            def _():
                to_mid(l, g, c).start()
            to_mate(l, g, c).start()

        def combine(l, g, c):
            @pl.when(mid == 1)
            def _():
                to_mid(l, g, c).wait_recv()
                for k in range(2):
                    b = (o_end, o_mid)[k]
                    own[l, g, c, b] = (own[l, g, c, b].astype(F32) + cmb[l, g, c, b - lo].astype(F32)).astype(BF16)
                    to_far(l, g, c, k).start()

        def finish(l, g, c):
            all_of(fin.at[l, g, c], rs_s, fn_r.at[l, g, c]).wait_recv()
            return (own[l, g, c, me].astype(F32) + fin[l, g, c, 0].astype(F32) + fin[l, g, c, 1].astype(F32)).astype(BF16)

        def x_phase(l, g):
            hrow = pl.ds(g * hb, hb)
            p_part = jnp.zeros((hb, rank + 2 * n_state), F32)
            for c in range(n_c):
                cols = pl.ds(c * chunk, chunk)
                x_new = finish(l, g, c)
                xi[l, hrow, cols] = x_new
                val = x_new.astype(F32) * cw[l, 3:4, cols] + cb[l : l + 1, cols]
                for k in range(3):
                    val = val + cs[l, k, hrow, cols].astype(F32) * cw[l, k : k + 1, cols]
                x_act = (val * jax.nn.sigmoid(val)).astype(BF16)
                xc[g, :, cols] = x_act.astype(F32)
                p_part = p_part + lax.dot_general(x_act, wx[l, :, cols], (((1,), (1,)), ((), ())), preferred_element_type=F32)
            pown[l, g] = p_part.astype(BF16)
            for j in range(1, n_ty):
                p_copy(l, g, j).start()

        def d_phase(l, g):
            p_sum = pown[l, g].astype(F32)
            all_of(pin.at[l, g], p_s, p_r.at[l, g]).wait_recv()
            for j in range(n_ty - 1):
                p_sum = p_sum + pin[l, g, j].astype(F32)
            dt_low = p_sum[:, :rank]
            dt_low = (dt_low * lax.rsqrt(jnp.mean(dt_low * dt_low, axis=-1, keepdims=True) + INNER_EPS)).astype(BF16)
            for i in range(2):
                mat = p_sum[:, rank + i * n_state : rank + (i + 1) * n_state]
                mat_t = (mat * lax.rsqrt(jnp.mean(mat * mat, axis=-1, keepdims=True) + INNER_EPS)).T
                for b in range(hb):
                    bc[i, b] = jnp.broadcast_to(mat_t[:, b : b + 1], (n_state, 128))
            for c in range(n_c):
                cols = pl.ds(c * chunk, chunk)
                raw = dot(dt_low, wdt[l, :, cols]) + db[l : l + 1, cols]
                delta = jnp.maximum(raw, 0.0) + jnp.log1p(jnp.exp(-jnp.abs(raw)))
                dt[:, cols] = delta
                dx[:, cols] = delta * xc[g, :, cols]
                neg_a = al[l, :, cols]

                def row_step(b, carry):
                    row = pl.ds(b, 1)
                    b_row = jnp.concatenate([bc[0, b]] * (chunk // 128), axis=1)
                    c_row = jnp.concatenate([bc[1, b]] * (chunk // 128), axis=1)
                    at = g * hb + b
                    s_new = jnp.exp2(dt[row, cols] * neg_a) * ss[l, at, :, cols] + dx[row, cols] * b_row
                    ss[l, at, :, cols] = s_new
                    sv[g, row, cols] = jnp.sum(s_new * c_row, axis=0, keepdims=True)
                    return carry

                lax.fori_loop(0, hb, row_step, 0, unroll=4)

        def y_phase(l, g, c):
            cols = pl.ds(c * chunk, chunk)
            z_new = finish(l, g, n_c + c).astype(F32)
            y = (sv[g, :, cols] + ds[l : l + 1, cols] * xc[g, :, cols]) * (z_new * jax.nn.sigmoid(z_new))
            yall[l, g, c, me] = y.astype(BF16)

            @pl.when(mid == 0)
            def _():
                ag_copy(l, g, c, me, 0, o_mid).start()

            ag_copy(l, g, c, me, 1, mate).start()

            @pl.when(mid == 1)
            def _():
                ag_copy(l, g, c, me, 1, o_end).start()
                ag_copy(l, g, c, me, 1, o_mid).start()

        def gather(l, g, c):
            @pl.when(mid == 1)
            def _():
                ag_copy(l, g, c, o_end, 0, mate).wait_recv()
                ag_copy(l, g, c, o_end, 0, mate).start()

        def w_phase(l, g, c):
            @pl.when(mid == 0)
            def _():
                ag_copy(l, g, c, o_end, 0, mate).wait_recv()
            all_of(yall.at[l, g, c, pl.ds(0, 2)], ag_s, ag_r.at[l, g, c, 1]).wait_recv()
            y_all = yall[l, g, c].reshape(rg, chunk)
            for q in range(n_q):
                qc = pl.ds(q * qw, qw)
                out = dot(y_all, wout[l, pl.ds(c * chunk, chunk), qc])
                acc[g, :, qc] = out if c == 0 else acc[g, :, qc] + out
                if c == n_c - 1:
                    so[0, l, g, q] = acc[g, other, qc].astype(BF16)
                    s_copy(0, l, g, q).start()

        def sum_1(l, g):
            for q in range(n_q):
                s_copy(0, l, g, q).wait_recv()
                so[1, l, g, q] = (acc[g, mine, pl.ds(q * qw, qw)] + si[0, l, g, q].astype(F32)).astype(BF16)
                s_copy(1, l, g, q).start()

        def sum_2(l, g):
            for q in range(n_q):
                qc = pl.ds(q * qw, qw)
                s_copy(1, l, g, q).wait_recv()
                tot = (so[1, l, g, q].astype(F32) + si[1, l, g, q].astype(F32)).astype(BF16)
                so[2, l, g, q] = tot
                s_copy(2, l, g, q).start()
                r[g, mine, qc] += tot.astype(F32)

        def sum_3(l, g):
            for q in range(n_q):
                s_copy(2, l, g, q).wait_recv()
                r[g, other, pl.ds(q * qw, qw)] += si[2, l, g, q].astype(F32)

        ph = dict(
            stat=stat, head=head, send=send, c=combine, x=x_phase, d=d_phase,
            y=y_phase, g=gather, w=w_phase, s1=sum_1, s2=sum_2, s3=sum_3,
        )

        def run(name, *args):
            with jax.named_scope(name + "_" + "_".join(map(str, args))):
                ph[name](*args)

        def proj(l, g, c):
            with jax.named_scope(f"proj_{l}_{g}_{c}"):
                project(l, (g,), c)
            send(l, g, c)

        groups, A, B = range(n_g), 0, 1
        for g in groups:
            start(*[("r", g, b) for b in range(n_tx)])
        start("nw")
        for k in range(1, n_tx):
            pl.semaphore_signal(barrier, 1, device_id=tx_of(lax.rem(me + k, n_tx)), device_id_type=MESH)
            pl.semaphore_signal(barrier, 1, device_id=(dp, lax.rem(me + k, n_tx), partner_ty), device_id_type=MESH)
        for k in range(1, n_ty):
            pl.semaphore_signal(barrier, 1, device_id=ty_of(lax.rem(ty + k, n_ty)), device_id_type=MESH)
        for g in groups:
            wait(*[("r", g, b) for b in range(n_tx)])
        wait("nw")
        start(*[("win", 0, t) for t in range(n_w)])
        pl.semaphore_wait(barrier, 2 * (n_tx - 1) + n_ty - 1)
        for g in groups:
            run("stat", 0, g)
        start("cw", "cb", "db", "al", "ds", "cs", ("wx", 0), ("wdt", 0), ("ss", 0), ("wout", 0))
        def each(name, l, g, *cs):
            for c in cs:
                run(name, l, g, c)

        for l in range(n_layer):
            p = l - 1
            run("head", l, A)
            proj(l, A, 0)
            if l == 0:
                proj(l, A, 1)
                proj(l, A, 2)
                each("c", l, A, 0)
                proj(l, A, 3)
                each("send", l, A, 4, 5, 6, 7)
                run("head", l, B)
                proj(l, B, 0)
                each("c", l, A, 1, 2)
                proj(l, B, 1)
                each("c", l, A, 3)
                proj(l, B, 2)
                start(*[("win", 1, t) for t in range(n_w)])
                start(("wx", 1), ("wdt", 1), ("ss", 1), ("wout", 1))
                wait("cw", "cb", "db", "al", "ds", "cs", ("wx", 0))
                al[...] = -jnp.exp(al[...]) * LOG2E
                each("c", l, A, 4)
                proj(l, B, 3)
                each("send", l, B, 4, 5)
                each("c", l, A, 5)
                run("x", l, A)
                each("c", l, A, 6, 7)
                each("c", l, B, 0, 1)
            else:
                proj(l, A, 1)
                each("g", p, B, 0, 1, 2, 3)
                proj(l, A, 2)
                each("w", p, B, 0, 1, 2, 3)
                proj(l, A, 3)
                each("c", l, A, 0)
                run("s1", p, B)
                each("c", l, A, 1, 2)
                run("s2", p, B)
                run("stat", l, B)
                each("send", l, A, 4, 5, 6, 7)
                each("c", l, A, 3)
                run("s3", p, B)
                wait(("wx", l))
                run("x", l, A)
                run("head", l, B)
                proj(l, B, 0)
                each("c", l, A, 4)
                proj(l, B, 1)
                each("c", l, A, 5, 6)
                proj(l, B, 2)
                each("c", l, A, 7)
                each("c", l, B, 0)
                proj(l, B, 3)
                each("send", l, B, 4, 5)
                each("c", l, B, 1)
            wait(("wdt", l), ("ss", l))
            run("d", l, A)
            each("c", l, B, 2, 3)
            each("y", l, A, 0, 1, 2, 3)
            each("send", l, B, 6, 7)
            if l == 0:
                each("c", l, B, 4)
                each("g", l, A, 0, 1, 2, 3)
                run("x", l, B)
            else:
                run("x", l, B)
                each("c", l, B, 4)
                each("g", l, A, 0, 1, 2, 3)
            each("c", l, B, 5, 6, 7)
            wait(("wout", l))
            if l == 0:
                each("w", l, A, 0, 1, 2, 3)
                run("s1", l, A)
                run("d", l, B)
                run("s2", l, A)
                run("stat", l + 1, A)
                each("y", l, B, 0, 1, 2, 3)
                run("s3", l, A)
            else:
                run("d", l, B)
                each("y", l, B, 0, 1, 2, 3)
                each("w", l, A, 0, 1, 2, 3)
                run("s1", l, A)
        p = n_layer - 1
        each("g", p, B, 0, 1)
        each("w", p, B, 0)
        each("g", p, B, 2)
        each("w", p, B, 1)
        each("g", p, B, 3)
        run("s2", p, A)
        each("w", p, B, 2, 3)
        run("s3", p, A)
        run("s1", p, B)
        run("s2", p, B)
        run("s3", p, B)

        with jax.named_scope("end"):
            all_of(own.at[:, :, :, pl.ds(0, 3)], rs_s, fn_r.at[0, 0, 0]).wait_send()
            all_of(sti, st_s, fn_r.at[0, 0, 0]).wait_send()
            all_of(pin, p_s, fn_r.at[0, 0, 0]).wait_send()
            all_of(so, s_s, fn_r.at[0, 0, 0]).wait_send()

            @pl.when(mid == 0)
            def _():
                all_of(yall.at[:, :, :, pl.ds(0, 2)], ag_s, fn_r.at[0, 0, 0]).wait_send()

            @pl.when(mid == 1)
            def _():
                all_of(yall, ag_s, fn_r.at[0, 0, 0]).wait_send()

    def dma(*s):
        return pltpu.SemaphoreType.DMA(s) if s else pltpu.SemaphoreType.DMA

    def vm(t, *s):
        return pltpu.VMEM(s, t)

    nl, p_w = n_layer, rank + 2 * n_state
    scratch = [
        vm(F32, nl, d_loc), vm(BF16, nl, n_w, d_loc, 2, 128), vm(F32, nl, 4, chan), vm(F32, nl, chan),
        vm(BF16, nl, p_w, chan), vm(BF16, nl, rank, chan), vm(F32, nl, chan), vm(F32, nl, n_state, chan), vm(F32, nl, chan),
        vm(BF16, nl, chan, d_loc),
        vm(BF16, n_g, 2 * rg, 2 * d_loc), vm(BF16, nl, n_g, 2 * n_c, n_tx, hb, chunk),
        vm(BF16, nl, n_g, 2 * n_c, 2, hb, chunk), vm(BF16, nl, n_g, 2 * n_c, 2, hb, chunk),
        vm(F32, n_g, hb, chan), vm(F32, hb, chan), vm(F32, hb, chan), vm(F32, n_g, hb, chan),
        vm(F32, 2, hb, n_state, 128), vm(BF16, nl, n_g, hb, p_w), vm(BF16, nl, n_g, n_ty - 1, hb, p_w),
        vm(BF16, nl, n_g, n_c, n_tx, hb, chunk), vm(F32, n_g, rg, d_loc),
        vm(BF16, 3, nl, n_g, n_q, half, qw), vm(BF16, 3, nl, n_g, n_q, half, qw),
        vm(F32, nl, n_g, 8, half), vm(F32, nl, n_g, 2 * n_tx - 1, 8, half), vm(F32, rg, 128),
        dma(7 + 4 * nl), dma(n_g, n_tx), dma(nl, n_w),
        dma(), dma(nl, n_g, 2 * n_c), dma(nl, n_g, 2 * n_c),
        dma(), dma(nl, n_g), dma(), dma(nl, n_g, n_c, 2),
        dma(), dma(nl, n_g, 3, n_q), dma(), dma(nl, n_g),
    ]
    outs = (vm(F32, n_g, rg, d_loc), vm(BF16, nl, blk, chan), vm(BF16, nl, 3, blk, chan), vm(F32, nl, blk, n_state, chan))
    return kernel, outs, scratch


def store_kernel(r, xi, cs, ss, r_out, conv_out, ssm_out, sem):
    n_g, rg, _ = r.shape
    nl, blk = ss.shape[:2]
    hb = blk // n_g
    pairs = []
    for l in range(nl):
        for i in range(0, blk, 8):
            pairs.append((ss.at[l, pl.ds(i, 8)], ssm_out.at[l, pl.ds(i, 8)]))
    for l in range(nl):
        pairs.append((cs.at[l, pl.ds(1, 2)], conv_out.at[l, pl.ds(0, 2)]))
        pairs.append((xi.at[l], conv_out.at[l, 2]))
    for g in range(n_g):
        for b in range(rg // hb):
            pairs.append((r.at[g, pl.ds(b * hb, hb)], r_out.at[pl.ds(b * blk + g * hb, hb)]))
    copies = [pltpu.make_async_copy(src, dst, sem.at[i]) for i, (src, dst) in enumerate(pairs)]
    for cp in copies:
        cp.start()
    for cp in copies:
        cp.wait()


def solution(mesh):
    n_tx, n_ty = mesh.shape["tx"], mesh.shape["ty"]

    def local_step(residual, norm_w, w_in, conv_w, conv_b, w_x, w_dt, dt_bias, a_log, d_skip, w_out, conv_state, ssm_state):
        rows, d_loc = residual.shape
        n_layer, _, _, chan = w_in.shape
        rank, n_state = w_dt.shape[1], a_log.shape[-1]
        blk = rows // n_tx
        kernel, outs, scratch = make_kernel(n_layer, n_tx, n_ty, rows, d_loc, chan, rank, n_state, 512, 2, 2)
        parts = pl.pallas_call(
            kernel,
            out_shape=outs,
            in_specs=[ANY] * 13,
            out_specs=(VMEM,) * 4,
            scratch_shapes=scratch,
            compiler_params=pltpu.CompilerParams(collective_id=0, has_side_effects=True, vmem_limit_bytes=67043328 - 11 * 2**20),
            name="mixer",
        )(
            residual, norm_w, w_in, conv_w.transpose(0, 2, 1), conv_b, w_x.transpose(0, 2, 1), w_dt, dt_bias,
            a_log.transpose(0, 2, 1), d_skip, w_out, conv_state.transpose(0, 3, 1, 2), ssm_state.transpose(0, 1, 3, 2),
        )
        r_out, conv_out, ssm_out = pl.pallas_call(
            store_kernel,
            out_shape=(
                jax.ShapeDtypeStruct((rows, d_loc), F32),
                jax.ShapeDtypeStruct((n_layer, 3, blk, chan), BF16),
                jax.ShapeDtypeStruct((n_layer, blk, n_state, chan), F32),
            ),
            in_specs=[VMEM] * 4,
            out_specs=(ANY,) * 3,
            scratch_shapes=[pltpu.SemaphoreType.DMA((64,))],
            compiler_params=pltpu.CompilerParams(vmem_limit_bytes=12 * 2**20),
            name="store",
        )(*parts)
        return r_out, conv_out.transpose(0, 2, 3, 1), ssm_out.transpose(0, 1, 3, 2)

    cache_spec = P(None, ("dp", "tx"), "ty", None)
    in_specs = (P("dp", "tx"), P(None, "tx"), P(None, "tx", None, "ty"), P(None, "ty", None), P(None, "ty"), P(None, "ty", None), P(None, None, "ty"), P(None, "ty"), P(None, "ty", None), P(None, "ty"), P(None, "ty", "tx"), cache_spec, cache_spec)
    out_specs = (P("dp", "tx"), cache_spec, cache_spec)
    return jax.shard_map(local_step, mesh=mesh, in_specs=in_specs, out_specs=out_specs, check_vma=False)
```

```python
import jax
import jax.numpy as jnp
from jax import lax
from jax.experimental import pallas as pl
from jax.experimental.pallas import tpu as pltpu
from jax.sharding import PartitionSpec as P

NORM_EPS = 1e-5
INNER_EPS = 1e-6
LOG2E = 1.4426950408889634
BF16, F32 = jnp.bfloat16, jnp.float32
MESH = pl.DeviceIdType.MESH
ANY = pl.BlockSpec(memory_space=pl.ANY)
VMEM = pl.BlockSpec(memory_space=pltpu.VMEM)


def dot(a, b):
    return jnp.dot(a, b, preferred_element_type=F32)


def make_kernel(n_layer, n_tx, n_ty, rows, d_loc, chan, rank, n_state, chunk, n_g, n_q):
    blk = rows // n_tx
    hb = blk // n_g
    rg = n_tx * hb
    half = rg // 2
    n_c = chan // chunk
    d_model = d_loc * n_tx
    qw = d_loc // n_q
    n_w = chan // 128

    def kernel(
        r_hbm, nw_hbm, win_hbm, cw_hbm, cb_hbm, wx_hbm, wdt_hbm, db_hbm, al_hbm, ds_hbm, wout_hbm, cs_hbm, ss_hbm,
        r, xi, cs, ss,
        nw, win, cw, cb, wx, wdt, db, al, ds, wout,
        hx, own, cmb, fin, xc, dt, dx, sv, bc, dl, pown, pin, yall, acc, so, si, sto, sti, sc, sl, pf,
        ld_sem, r_sem, win_sem, rs_s, cm_r, fn_r, p_s, p_r, ag_s, ag_r, s_s, s_r, st_s, st_r,
    ):
        dp, me, ty = lax.axis_index("dp"), lax.axis_index("tx"), lax.axis_index("ty")
        core = lax.rem(ty, 2)
        mate = me + 1 - 2 * lax.rem(me, 2)
        mid = (me * (3 - me)) // 2
        o_end = 3 - me + mid * (me - mate)
        o_mid = 3 - mate + mid * (mate - me)
        lo = 2 * (1 - me // 2)
        barrier = pltpu.get_barrier_semaphore()

        def tx_of(k):
            return (dp, k, ty)

        def ty_of(k):
            return (dp, me, k)

        def remote(src, dst, ssem, rsem, dev):
            return pltpu.make_async_remote_copy(src_ref=src, dst_ref=dst, send_sem=ssem, recv_sem=rsem, device_id=dev, device_id_type=MESH)

        loads = {}
        for g in range(n_g):
            for b in range(n_tx):
                loads["r", g, b] = pltpu.make_async_copy(r_hbm.at[pl.ds(b * blk + g * hb, hb)], r.at[g, pl.ds(b * hb, hb)], r_sem.at[g, b])
        names = dict(nw=(nw_hbm, nw), cw=(cw_hbm, cw), cb=(cb_hbm, cb), db=(db_hbm, db), al=(al_hbm, al), ds=(ds_hbm, ds), cs=(cs_hbm, cs))
        for k, key in enumerate(names):
            loads[key] = pltpu.make_async_copy(names[key][0], names[key][1], ld_sem.at[k])
        for l in range(n_layer):
            for k, (key, src, dst) in enumerate((("wx", wx_hbm, wx), ("wdt", wdt_hbm, wdt), ("wout", wout_hbm, wout), ("ss", ss_hbm, ss))):
                loads[key, l] = pltpu.make_async_copy(src.at[l], dst.at[l], ld_sem.at[len(names) + 4 * l + k])
            for t in range(n_w):
                loads["win", l, t] = pltpu.make_async_copy(win_hbm.at[l, :, :, pl.ds(t * 128, 128)], win.at[l, t], win_sem.at[l, t])

        def start(*keys):
            for key in keys:
                loads[key].start()

        def wait(*keys):
            for key in keys:
                loads[key].wait()

        partner_ty = ty + 1 - 2 * core
        partner = ty_of(partner_ty)
        across = ty_of(lax.rem(ty + 2, n_ty))
        mine = pl.ds(pl.multiple_of(core * half, half), half)
        other = pl.ds(pl.multiple_of((1 - core) * half, half), half)

        def stat_copy(l, g, j, rel):
            dev = (dp, lax.rem(me + j, n_tx), partner_ty if rel else ty)
            return remote(sto.at[l, g], sti.at[l, g, 2 * j + rel - 1], st_s, st_r.at[l, g], dev)

        def to_mate(l, g, c):
            return remote(own.at[l, g, c, mate], fin.at[l, g, c, 0], rs_s, fn_r.at[l, g, c], tx_of(mate))

        def to_mid(l, g, c):
            return remote(own.at[l, g, c, pl.ds(lo, 2)], cmb.at[l, g, c], rs_s, cm_r.at[l, g, c], tx_of(mate))

        def to_far(l, g, c, k):
            b = (o_end, o_mid)[k]
            return remote(own.at[l, g, c, b], fin.at[l, g, c, 1], rs_s, fn_r.at[l, g, c], tx_of(b))

        def p_copy(l, g, j):
            return remote(pown.at[l, g], pin.at[l, g, j - 1], p_s, p_r.at[l, g], ty_of(lax.rem(ty + j, n_ty)))

        def ag_copy(l, g, c, b, k, dev):
            return remote(yall.at[l, g, c, b], yall.at[l, g, c, b], ag_s, ag_r.at[l, g, c, k], tx_of(dev))

        def s_copy(i, l, g, q):
            return remote(so.at[i, l, g, q], si.at[i, l, g, q], s_s, s_r.at[l, g, i, q], across if i == 1 else partner)

        def all_of(ref, ssem, rsem):
            return remote(ref, ref, ssem, rsem, partner)

        def stat(l, g):
            part = r[g, mine, :]
            sq = jnp.sum(part * part, axis=-1, keepdims=True)
            sto[l, g] = jnp.broadcast_to(sq, (half, 128)).T[0:8, :]
            for j in range(n_tx - 1, -1, -1):
                for rel in range(2):
                    if j or rel:
                        stat_copy(l, g, j, rel).start()

        def head(l, g):
            for b in range(2):
                at = pl.ds(b * half, half)
                part = r[g, at, :]
                sq = jnp.sum(part * part, axis=-1, keepdims=True)
                sl[g, at, :] = lax.rsqrt(jnp.broadcast_to(sq, (half, 128)) / d_model + NORM_EPS)
            scale = sl[g]
            row_i = lax.broadcasted_iota(jnp.int32, (128, 256), 0)
            col_i = lax.broadcasted_iota(jnp.int32, (128, 256), 1)
            pick = [(col_i == 2 * row_i + k).astype(F32).astype(BF16) for k in range(2)]
            for j in range(d_loc // 128):
                cols = pl.ds(j * 128, 128)
                h = (r[g, :, cols] * scale * nw[l : l + 1, cols]).astype(BF16)
                for k in range(2):
                    hx[g, k * rg : (k + 1) * rg, pl.ds(j * 256, 256)] = dot(h, pick[k]).astype(BF16)

        def norm(l, g):
            all_of(sti.at[l, g], st_s, st_r.at[l, g]).wait_recv()
            for rel, at in enumerate((mine, other)):
                tot = sto[l, g] if rel == 0 else sti[l, g, 0]
                for j in range(1, n_tx):
                    tot = tot + sti[l, g, 2 * j + rel - 1]
                sc[at, :] = lax.rsqrt(jnp.broadcast_to(tot[0:1, :], (128, half)).T / d_model + NORM_EPS)
            sl[g] = jnp.where(sl[g] > 0.0, sc[...] / sl[g], 0.0)

        def project(l, g, c, early):
            for t in range(0, chunk // 128, 2):
                tile = c * (chunk // 128) + t
                w = jnp.concatenate([win.at[l, tile + i].reshape(2 * d_loc, 128)[...] for i in range(2)], axis=1)
                part = dot(hx[g], w)
                if early:
                    pf[c, :, pl.ds(t * 128, 256)] = part
                else:
                    scaled(l, g, c, t, part)

        def scaled(l, g, c, t, part):
            ratio = jnp.concatenate([sl[g], sl[g]], axis=1)
            for k in range(2):
                piece = (part[k * rg : (k + 1) * rg, :] * ratio).astype(BF16)
                for b in range(n_tx):
                    own[l, g, k * n_c + c, b, :, pl.ds(t * 128, 256)] = piece[b * hb : (b + 1) * hb, :]

        def out(l, g, c):
            for t in range(0, chunk // 128, 2):
                scaled(l, g, c, t, pf[c, :, pl.ds(t * 128, 256)])
            send(l, g, c)

        def send(l, g, c):
            @pl.when(mid == 0)
            def _():
                to_mid(l, g, c).start()
            to_mate(l, g, c).start()

        def combine(l, g, c):
            @pl.when(mid == 1)
            def _():
                to_mid(l, g, c).wait_recv()
                for k in range(2):
                    b = (o_end, o_mid)[k]
                    own[l, g, c, b] = (own[l, g, c, b].astype(F32) + cmb[l, g, c, b - lo].astype(F32)).astype(BF16)
                    to_far(l, g, c, k).start()

        def finish(l, g, c):
            all_of(fin.at[l, g, c], rs_s, fn_r.at[l, g, c]).wait_recv()
            return (own[l, g, c, me].astype(F32) + fin[l, g, c, 0].astype(F32) + fin[l, g, c, 1].astype(F32)).astype(BF16)

        def x_phase(l, g):
            hrow = pl.ds(g * hb, hb)
            p_part = jnp.zeros((hb, rank + 2 * n_state), F32)
            for c in range(n_c):
                cols = pl.ds(c * chunk, chunk)
                x_new = finish(l, g, c)
                xi[l, hrow, cols] = x_new
                val = x_new.astype(F32) * cw[l, 3:4, cols] + cb[l : l + 1, cols]
                for k in range(3):
                    val = val + cs[l, k, hrow, cols].astype(F32) * cw[l, k : k + 1, cols]
                x_act = (val * jax.nn.sigmoid(val)).astype(BF16)
                xc[g, :, cols] = x_act.astype(F32)
                p_part = p_part + lax.dot_general(x_act, wx[l, :, cols], (((1,), (1,)), ((), ())), preferred_element_type=F32)
            pown[l, g] = p_part.astype(BF16)
            for j in range(1, n_ty):
                p_copy(l, g, j).start()

        def d_phase(l, g):
            p_sum = pown[l, g].astype(F32)
            all_of(pin.at[l, g], p_s, p_r.at[l, g]).wait_recv()
            for j in range(n_ty - 1):
                p_sum = p_sum + pin[l, g, j].astype(F32)
            dt_low = p_sum[:, :rank]
            dt_low = (dt_low * lax.rsqrt(jnp.mean(dt_low * dt_low, axis=-1, keepdims=True) + INNER_EPS)).astype(BF16)
            for i in range(2):
                mat = p_sum[:, rank + i * n_state : rank + (i + 1) * n_state]
                mat_t = (mat * lax.rsqrt(jnp.mean(mat * mat, axis=-1, keepdims=True) + INNER_EPS)).T
                for b in range(hb):
                    bc[g, i, b] = jnp.broadcast_to(mat_t[:, b : b + 1], (n_state, 128))
            dl[g] = dt_low

        def d_chunk(l, g, c):
            cols = pl.ds(c * chunk, chunk)
            dt_low = dl[g]
            raw = dot(dt_low, wdt[l, :, cols]) + db[l : l + 1, cols]
            delta = jnp.maximum(raw, 0.0) + jnp.log1p(jnp.exp(-jnp.abs(raw)))
            dt[:, cols] = delta
            dx[:, cols] = delta * xc[g, :, cols]
            neg_a = al[l, :, cols]

            def row_step(b, carry):
                row = pl.ds(b, 1)
                b_row = jnp.concatenate([bc[g, 0, b]] * (chunk // 128), axis=1)
                c_row = jnp.concatenate([bc[g, 1, b]] * (chunk // 128), axis=1)
                at = g * hb + b
                s_new = jnp.exp2(dt[row, cols] * neg_a) * ss[l, at, :, cols] + dx[row, cols] * b_row
                ss[l, at, :, cols] = s_new
                sv[g, row, cols] = jnp.sum(s_new * c_row, axis=0, keepdims=True)
                return carry

            lax.fori_loop(0, hb, row_step, 0, unroll=4)

        def y_phase(l, g, c):
            cols = pl.ds(c * chunk, chunk)
            z_new = finish(l, g, n_c + c).astype(F32)
            y = (sv[g, :, cols] + ds[l : l + 1, cols] * xc[g, :, cols]) * (z_new * jax.nn.sigmoid(z_new))
            yall[l, g, c, me] = y.astype(BF16)

            @pl.when(mid == 0)
            def _():
                ag_copy(l, g, c, me, 0, o_mid).start()

            @pl.when(mid == 1)
            def _():
                ag_copy(l, g, c, me, 1, o_end).start()
                ag_copy(l, g, c, me, 1, o_mid).start()

        def y_mate(l, g):
            for c in range(n_c):
                ag_copy(l, g, c, me, 1, mate).start()

        def gather(l, g, c):
            @pl.when(mid == 1)
            def _():
                ag_copy(l, g, c, o_end, 0, mate).wait_recv()
                ag_copy(l, g, c, o_end, 0, mate).start()

        def w_phase(l, g, c):
            @pl.when(mid == 0)
            def _():
                ag_copy(l, g, c, o_end, 0, mate).wait_recv()
            all_of(yall.at[l, g, c, pl.ds(0, 2)], ag_s, ag_r.at[l, g, c, 1]).wait_recv()
            y_all = yall[l, g, c].reshape(rg, chunk)
            for q in range(n_q):
                qc = pl.ds(q * qw, qw)
                out = dot(y_all, wout[l, pl.ds(c * chunk, chunk), qc])
                acc[g, :, qc] = out if c == 0 else acc[g, :, qc] + out
                if c == n_c - 1:
                    so[0, l, g, q] = acc[g, other, qc].astype(BF16)
                    s_copy(0, l, g, q).start()

        def sum_1(l, g):
            for q in range(n_q):
                s_copy(0, l, g, q).wait_recv()
                so[1, l, g, q] = (acc[g, mine, pl.ds(q * qw, qw)] + si[0, l, g, q].astype(F32)).astype(BF16)
                s_copy(1, l, g, q).start()

        def sum_2(l, g):
            for q in range(n_q):
                qc = pl.ds(q * qw, qw)
                s_copy(1, l, g, q).wait_recv()
                tot = (so[1, l, g, q].astype(F32) + si[1, l, g, q].astype(F32)).astype(BF16)
                so[2, l, g, q] = tot
                s_copy(2, l, g, q).start()
                r[g, mine, qc] += tot.astype(F32)

        def sum_3(l, g):
            for q in range(n_q):
                s_copy(2, l, g, q).wait_recv()
                r[g, other, pl.ds(q * qw, qw)] += si[2, l, g, q].astype(F32)

        ph = dict(
            stat=stat, head=head, norm=norm, out=out, send=send, c=combine, x=x_phase, d=d_phase, dc=d_chunk,
            y=y_phase, ym=y_mate, g=gather, w=w_phase, s1=sum_1, s2=sum_2, s3=sum_3,
        )

        def run(name, *args):
            with jax.named_scope(name + "_" + "_".join(map(str, args))):
                ph[name](*args)

        def proj(l, g, c, early=False):
            with jax.named_scope(f"proj_{l}_{g}_{c}"):
                project(l, g, c, early)
            if not early:
                send(l, g, c)

        groups, A, B = range(n_g), 0, 1
        for g in groups:
            start(*[("r", g, b) for b in range(n_tx)])
        start("nw")
        for k in range(1, n_tx):
            pl.semaphore_signal(barrier, 1, device_id=tx_of(lax.rem(me + k, n_tx)), device_id_type=MESH)
            pl.semaphore_signal(barrier, 1, device_id=(dp, lax.rem(me + k, n_tx), partner_ty), device_id_type=MESH)
        for k in range(1, n_ty):
            pl.semaphore_signal(barrier, 1, device_id=ty_of(lax.rem(ty + k, n_ty)), device_id_type=MESH)
        for g in groups:
            wait(*[("r", g, b) for b in range(n_tx)])
        wait("nw")
        start(*[("win", 0, t) for t in range(n_w)])
        pl.semaphore_wait(barrier, 2 * (n_tx - 1) + n_ty - 1)
        for g in groups:
            run("stat", 0, g)
        start("cw", "cb", "db", "al", "ds", "cs", ("wx", 0), ("wdt", 0), ("ss", 0), ("wout", 0))
        def each(name, l, g, *cs):
            for c in cs:
                run(name, l, g, c)

        def d_all(l, g):
            run("d", l, g)
            each("dc", l, g, 0, 1, 2, 3)

        run("head", 0, A)
        wait(*[("win", 0, t) for t in range(n_w // 2)])
        proj(0, A, 0, True)
        proj(0, A, 1, True)
        run("norm", 0, A)
        each("out", 0, A, 0, 1)
        wait(*[("win", 0, t) for t in range(n_w // 2, n_w)])
        proj(0, A, 2)
        proj(0, A, 3)
        each("send", 0, A, 4, 5, 6, 7)
        run("head", 0, B)
        run("norm", 0, B)
        each("c", 0, A, 0)
        proj(0, B, 0)
        each("c", 0, A, 1)
        proj(0, B, 1)
        each("c", 0, A, 2)
        proj(0, B, 2)
        start(*[("win", 1, t) for t in range(n_w)])
        start(("wx", 1), ("wdt", 1), ("ss", 1), ("wout", 1))
        wait("cw", "cb", "db", "al", "ds", "cs", ("wx", 0))
        al[...] = -jnp.exp(al[...]) * LOG2E
        each("c", 0, A, 3)
        proj(0, B, 3)
        each("send", 0, B, 4)
        each("c", 0, A, 4, 5)
        run("x", 0, A)
        each("c", 0, A, 6, 7)
        each("c", 0, B, 0, 1)
        wait(("wdt", 0), ("ss", 0))
        run("d", 0, A)
        each("dc", 0, A, 0, 1)
        each("c", 0, B, 2)
        each("dc", 0, A, 2, 3)
        each("c", 0, B, 3)
        each("y", 0, A, 0, 1, 2, 3)
        run("ym", 0, A)
        each("send", 0, B, 5, 6, 7)
        each("c", 0, B, 4)
        each("g", 0, A, 0, 1)
        run("x", 0, B)
        each("g", 0, A, 2, 3)
        each("c", 0, B, 5, 6, 7)
        wait(("wout", 0))
        each("w", 0, A, 0, 1, 2, 3)
        run("s1", 0, A)
        d_all(0, B)
        run("s2", 0, A)
        run("stat", 1, A)
        each("y", 0, B, 0, 1, 2, 3)
        run("ym", 0, B)
        run("s3", 0, A)
        wait(*[("win", 1, t) for t in range(n_w)])
        run("head", 1, A)
        proj(1, A, 0, True)
        proj(1, A, 1, True)
        run("norm", 1, A)
        each("out", 1, A, 0, 1)
        each("g", 0, B, 0, 1)
        proj(1, A, 2)
        each("g", 0, B, 2, 3)
        proj(1, A, 3)
        each("w", 0, B, 0, 1, 2, 3)
        each("c", 1, A, 0, 1)
        run("s1", 0, B)
        each("c", 1, A, 2, 3)
        run("s2", 0, B)
        run("stat", 1, B)
        each("send", 1, A, 4, 5, 6, 7)
        run("s3", 0, B)
        run("head", 1, B)
        proj(1, B, 0, True)
        proj(1, B, 1, True)
        wait(("wx", 1))
        run("x", 1, A)
        run("norm", 1, B)
        each("out", 1, B, 0, 1)
        proj(1, B, 2)
        each("c", 1, A, 4, 5)
        proj(1, B, 3)
        each("send", 1, B, 4, 5, 6, 7)
        each("c", 1, A, 6, 7)
        wait(("wdt", 1), ("ss", 1))
        run("d", 1, A)
        each("dc", 1, A, 0, 1)
        each("c", 1, B, 0)
        each("dc", 1, A, 2, 3)
        each("c", 1, B, 1, 2, 3)
        each("y", 1, A, 0, 1, 2, 3)
        run("ym", 1, A)
        each("c", 1, B, 4, 5)
        run("x", 1, B)
        each("c", 1, B, 6, 7)
        each("g", 1, A, 0, 1, 2, 3)
        run("d", 1, B)
        for c in range(n_c):
            run("dc", 1, B, c)
            run("y", 1, B, c)
        run("ym", 1, B)
        wait(("wout", 1))
        each("w", 1, A, 0, 1, 2, 3)
        each("g", 1, B, 0, 1)
        run("s1", 1, A)
        each("w", 1, B, 0)
        each("g", 1, B, 2)
        each("w", 1, B, 1)
        each("g", 1, B, 3)
        each("w", 1, B, 2, 3)
        run("s2", 1, A)
        run("s1", 1, B)
        run("s3", 1, A)
        run("s2", 1, B)
        run("s3", 1, B)

        with jax.named_scope("end"):
            all_of(own.at[:, :, :, pl.ds(0, 3)], rs_s, fn_r.at[0, 0, 0]).wait_send()
            all_of(sti, st_s, fn_r.at[0, 0, 0]).wait_send()
            all_of(pin, p_s, fn_r.at[0, 0, 0]).wait_send()
            all_of(so, s_s, fn_r.at[0, 0, 0]).wait_send()

            @pl.when(mid == 0)
            def _():
                all_of(yall.at[:, :, :, pl.ds(0, 2)], ag_s, fn_r.at[0, 0, 0]).wait_send()

            @pl.when(mid == 1)
            def _():
                all_of(yall, ag_s, fn_r.at[0, 0, 0]).wait_send()

    def dma(*s):
        return pltpu.SemaphoreType.DMA(s) if s else pltpu.SemaphoreType.DMA

    def vm(t, *s):
        return pltpu.VMEM(s, t)

    nl, p_w = n_layer, rank + 2 * n_state
    scratch = [
        vm(F32, nl, d_loc), vm(BF16, nl, n_w, d_loc, 2, 128), vm(F32, nl, 4, chan), vm(F32, nl, chan),
        vm(BF16, nl, p_w, chan), vm(BF16, nl, rank, chan), vm(F32, nl, chan), vm(F32, nl, n_state, chan), vm(F32, nl, chan),
        vm(BF16, nl, chan, d_loc),
        vm(BF16, n_g, 2 * rg, 2 * d_loc), vm(BF16, nl, n_g, 2 * n_c, n_tx, hb, chunk),
        vm(BF16, nl, n_g, 2 * n_c, 2, hb, chunk), vm(BF16, nl, n_g, 2 * n_c, 2, hb, chunk),
        vm(F32, n_g, hb, chan), vm(F32, hb, chan), vm(F32, hb, chan), vm(F32, n_g, hb, chan),
        vm(F32, n_g, 2, hb, n_state, 128), vm(BF16, n_g, hb, rank), vm(BF16, nl, n_g, hb, p_w), vm(BF16, nl, n_g, n_ty - 1, hb, p_w),
        vm(BF16, nl, n_g, n_c, n_tx, hb, chunk), vm(F32, n_g, rg, d_loc),
        vm(BF16, 3, nl, n_g, n_q, half, qw), vm(BF16, 3, nl, n_g, n_q, half, qw),
        vm(F32, nl, n_g, 8, half), vm(F32, nl, n_g, 2 * n_tx - 1, 8, half), vm(F32, rg, 128), vm(F32, n_g, rg, 128), vm(F32, 2, 2 * rg, chunk),
        dma(7 + 4 * nl), dma(n_g, n_tx), dma(nl, n_w),
        dma(), dma(nl, n_g, 2 * n_c), dma(nl, n_g, 2 * n_c),
        dma(), dma(nl, n_g), dma(), dma(nl, n_g, n_c, 2),
        dma(), dma(nl, n_g, 3, n_q), dma(), dma(nl, n_g),
    ]
    outs = (vm(F32, n_g, rg, d_loc), vm(BF16, nl, blk, chan), vm(BF16, nl, 3, blk, chan), vm(F32, nl, blk, n_state, chan))
    return kernel, outs, scratch


def store_kernel(r, xi, cs, ss, r_out, conv_out, ssm_out, sem):
    n_g, rg, _ = r.shape
    nl, blk = ss.shape[:2]
    hb = blk // n_g
    pairs = []
    for l in range(nl):
        for i in range(0, blk, 8):
            pairs.append((ss.at[l, pl.ds(i, 8)], ssm_out.at[l, pl.ds(i, 8)]))
    for l in range(nl):
        pairs.append((cs.at[l, pl.ds(1, 2)], conv_out.at[l, pl.ds(0, 2)]))
        pairs.append((xi.at[l], conv_out.at[l, 2]))
    for g in range(n_g):
        for b in range(rg // hb):
            pairs.append((r.at[g, pl.ds(b * hb, hb)], r_out.at[pl.ds(b * blk + g * hb, hb)]))
    copies = [pltpu.make_async_copy(src, dst, sem.at[i]) for i, (src, dst) in enumerate(pairs)]
    for cp in copies:
        cp.start()
    for cp in copies:
        cp.wait()


def solution(mesh):
    n_tx, n_ty = mesh.shape["tx"], mesh.shape["ty"]

    def local_step(residual, norm_w, w_in, conv_w, conv_b, w_x, w_dt, dt_bias, a_log, d_skip, w_out, conv_state, ssm_state):
        rows, d_loc = residual.shape
        n_layer, _, _, chan = w_in.shape
        rank, n_state = w_dt.shape[1], a_log.shape[-1]
        blk = rows // n_tx
        kernel, outs, scratch = make_kernel(n_layer, n_tx, n_ty, rows, d_loc, chan, rank, n_state, 512, 2, 2)
        parts = pl.pallas_call(
            kernel,
            out_shape=outs,
            in_specs=[ANY] * 13,
            out_specs=(VMEM,) * 4,
            scratch_shapes=scratch,
            compiler_params=pltpu.CompilerParams(collective_id=0, has_side_effects=True, vmem_limit_bytes=67043328 - 11 * 2**20),
            name="mixer",
        )(
            residual, norm_w, w_in, conv_w.transpose(0, 2, 1), conv_b, w_x.transpose(0, 2, 1), w_dt, dt_bias,
            a_log.transpose(0, 2, 1), d_skip, w_out, conv_state.transpose(0, 3, 1, 2), ssm_state.transpose(0, 1, 3, 2),
        )
        r_out, conv_out, ssm_out = pl.pallas_call(
            store_kernel,
            out_shape=(
                jax.ShapeDtypeStruct((rows, d_loc), F32),
                jax.ShapeDtypeStruct((n_layer, 3, blk, chan), BF16),
                jax.ShapeDtypeStruct((n_layer, blk, n_state, chan), F32),
            ),
            in_specs=[VMEM] * 4,
            out_specs=(ANY,) * 3,
            scratch_shapes=[pltpu.SemaphoreType.DMA((64,))],
            compiler_params=pltpu.CompilerParams(vmem_limit_bytes=12 * 2**20),
            name="store",
        )(*parts)
        return r_out, conv_out.transpose(0, 2, 3, 1), ssm_out.transpose(0, 1, 3, 2)

    cache_spec = P(None, ("dp", "tx"), "ty", None)
    in_specs = (P("dp", "tx"), P(None, "tx"), P(None, "tx", None, "ty"), P(None, "ty", None), P(None, "ty"), P(None, "ty", None), P(None, None, "ty"), P(None, "ty"), P(None, "ty", None), P(None, "ty"), P(None, "ty", "tx"), cache_spec, cache_spec)
    out_specs = (P("dp", "tx"), cache_spec, cache_spec)
    return jax.shard_map(local_step, mesh=mesh, in_specs=in_specs, out_specs=out_specs, check_vma=False)
```

```python
import jax
import jax.numpy as jnp
from jax import lax
from jax.experimental import pallas as pl
from jax.experimental.pallas import tpu as pltpu
from jax.sharding import PartitionSpec as P

NORM_EPS = 1e-5
INNER_EPS = 1e-6
LOG2E = 1.4426950408889634
BF16, F32 = jnp.bfloat16, jnp.float32
MESH = pl.DeviceIdType.MESH
ANY = pl.BlockSpec(memory_space=pl.ANY)
VMEM = pl.BlockSpec(memory_space=pltpu.VMEM)


def dot(a, b):
    return jnp.dot(a, b, preferred_element_type=F32)


def make_kernel(n_layer, n_tx, n_ty, rows, d_loc, chan, rank, n_state, chunk, n_g, n_q):
    blk = rows // n_tx
    hb = blk // n_g
    rg = n_tx * hb
    half = rg // 2
    n_c = chan // chunk
    d_model = d_loc * n_tx
    qw = d_loc // n_q
    n_w = chan // 128

    def kernel(
        r_hbm, nw_hbm, win_hbm, cw_hbm, cb_hbm, wx_hbm, wdt_hbm, db_hbm, al_hbm, ds_hbm, wout_hbm, cs_hbm, ss_hbm,
        r, xi, cs, ss,
        nw, win, cw, cb, wx, wdt, db, al, ds, wout,
        hx, own, cmb, fin, xc, dt, dx, sv, bc, dl, pown, pin, yall, acc, so, si, sto, sti, sc, sl, pf,
        ld_sem, r_sem, win_sem, rs_s, cm_r, fn_r, p_s, p_r, ag_s, ag_r, s_s, s_r, st_s, st_r,
    ):
        dp, me, ty = lax.axis_index("dp"), lax.axis_index("tx"), lax.axis_index("ty")
        core = lax.rem(ty, 2)
        mate = me + 1 - 2 * lax.rem(me, 2)
        mid = (me * (3 - me)) // 2
        o_end = 3 - me + mid * (me - mate)
        o_mid = 3 - mate + mid * (mate - me)
        lo = 2 * (1 - me // 2)
        barrier = pltpu.get_barrier_semaphore()

        def tx_of(k):
            return (dp, k, ty)

        def ty_of(k):
            return (dp, me, k)

        def remote(src, dst, ssem, rsem, dev):
            return pltpu.make_async_remote_copy(src_ref=src, dst_ref=dst, send_sem=ssem, recv_sem=rsem, device_id=dev, device_id_type=MESH)

        loads = {}
        for g in range(n_g):
            for b in range(n_tx):
                loads["r", g, b] = pltpu.make_async_copy(r_hbm.at[pl.ds(b * blk + g * hb, hb)], r.at[g, pl.ds(b * hb, hb)], r_sem.at[g, b])
        names = dict(nw=(nw_hbm, nw), cw=(cw_hbm, cw), cb=(cb_hbm, cb), db=(db_hbm, db), al=(al_hbm, al), ds=(ds_hbm, ds), cs=(cs_hbm, cs))
        for k, key in enumerate(names):
            loads[key] = pltpu.make_async_copy(names[key][0], names[key][1], ld_sem.at[k])
        for l in range(n_layer):
            for k, (key, src, dst) in enumerate((("wx", wx_hbm, wx), ("wdt", wdt_hbm, wdt), ("wout", wout_hbm, wout), ("ss", ss_hbm, ss))):
                loads[key, l] = pltpu.make_async_copy(src.at[l], dst.at[l], ld_sem.at[len(names) + 4 * l + k])
            for t in range(n_w):
                loads["win", l, t] = pltpu.make_async_copy(win_hbm.at[l, :, :, pl.ds(t * 128, 128)], win.at[l, t], win_sem.at[l, t])

        def start(*keys):
            for key in keys:
                loads[key].start()

        def wait(*keys):
            for key in keys:
                loads[key].wait()

        partner_ty = ty + 1 - 2 * core
        partner = ty_of(partner_ty)
        across = ty_of(lax.rem(ty + 2, n_ty))
        mine = pl.ds(pl.multiple_of(core * half, half), half)
        other = pl.ds(pl.multiple_of((1 - core) * half, half), half)

        def stat_copy(l, g, j, rel):
            dev = (dp, lax.rem(me + j, n_tx), partner_ty if rel else ty)
            return remote(sto.at[l, g], sti.at[l, g, 2 * j + rel - 1], st_s, st_r.at[l, g], dev)

        def to_mate(l, g, c):
            return remote(own.at[l, g, c, mate], fin.at[l, g, c, 0], rs_s, fn_r.at[l, g, c], tx_of(mate))

        def to_mid(l, g, c):
            return remote(own.at[l, g, c, pl.ds(lo, 2)], cmb.at[l, g, c], rs_s, cm_r.at[l, g, c], tx_of(mate))

        def to_far(l, g, c, k):
            b = (o_end, o_mid)[k]
            return remote(own.at[l, g, c, b], fin.at[l, g, c, 1], rs_s, fn_r.at[l, g, c], tx_of(b))

        def p_copy(l, g, j):
            return remote(pown.at[l, g], pin.at[l, g, j - 1], p_s, p_r.at[l, g], ty_of(lax.rem(ty + j, n_ty)))

        def ag_copy(l, g, c, b, k, dev):
            return remote(yall.at[l, g, c, b], yall.at[l, g, c, b], ag_s, ag_r.at[l, g, c, k], tx_of(dev))

        def s_copy(i, l, g, q):
            return remote(so.at[i, l, g, q], si.at[i, l, g, q], s_s, s_r.at[l, g, i, q], across if i == 1 else partner)

        def all_of(ref, ssem, rsem):
            return remote(ref, ref, ssem, rsem, partner)

        def stat(l, g):
            part = r[g, mine, :]
            sq = jnp.sum(part * part, axis=-1, keepdims=True)
            sto[l, g] = jnp.broadcast_to(sq, (half, 128)).T[0:8, :]
            for j in range(n_tx - 1, -1, -1):
                for rel in range(2):
                    if j or rel:
                        stat_copy(l, g, j, rel).start()

        def head(l, g):
            for b in range(2):
                at = pl.ds(b * half, half)
                part = r[g, at, :]
                sq = jnp.sum(part * part, axis=-1, keepdims=True)
                sl[g, at, :] = lax.rsqrt(jnp.broadcast_to(sq, (half, 128)) / d_model + NORM_EPS)
            scale = sl[g]
            row_i = lax.broadcasted_iota(jnp.int32, (128, 256), 0)
            col_i = lax.broadcasted_iota(jnp.int32, (128, 256), 1)
            pick = [(col_i == 2 * row_i + k).astype(F32).astype(BF16) for k in range(2)]
            for j in range(d_loc // 128):
                cols = pl.ds(j * 128, 128)
                h = (r[g, :, cols] * scale * nw[l : l + 1, cols]).astype(BF16)
                for k in range(2):
                    hx[g, k * rg : (k + 1) * rg, pl.ds(j * 256, 256)] = dot(h, pick[k]).astype(BF16)

        def norm(l, g):
            all_of(sti.at[l, g], st_s, st_r.at[l, g]).wait_recv()
            for rel, at in enumerate((mine, other)):
                tot = sto[l, g] if rel == 0 else sti[l, g, 0]
                for j in range(1, n_tx):
                    tot = tot + sti[l, g, 2 * j + rel - 1]
                sc[at, :] = lax.rsqrt(jnp.broadcast_to(tot[0:1, :], (128, half)).T / d_model + NORM_EPS)
            sl[g] = jnp.where(sl[g] > 0.0, sc[...] / sl[g], 0.0)

        def project(l, g, c, early):
            for t in range(0, chunk // 128, 2):
                tile = c * (chunk // 128) + t
                w = jnp.concatenate([win.at[l, tile + i].reshape(2 * d_loc, 128)[...] for i in range(2)], axis=1)
                part = dot(hx[g], w)
                if early:
                    pf[c, :, pl.ds(t * 128, 256)] = part
                else:
                    scaled(l, g, c, t, part)

        def scaled(l, g, c, t, part):
            ratio = jnp.concatenate([sl[g], sl[g]], axis=1)
            for k in range(2):
                piece = (part[k * rg : (k + 1) * rg, :] * ratio).astype(BF16)
                for b in range(n_tx):
                    own[l, g, k * n_c + c, b, :, pl.ds(t * 128, 256)] = piece[b * hb : (b + 1) * hb, :]

        def out(l, g, c):
            for t in range(0, chunk // 128, 2):
                scaled(l, g, c, t, pf[c, :, pl.ds(t * 128, 256)])
            send(l, g, c)

        def send(l, g, c):
            @pl.when(mid == 0)
            def _():
                to_mid(l, g, c).start()
            to_mate(l, g, c).start()

        def combine(l, g, c):
            @pl.when(mid == 1)
            def _():
                to_mid(l, g, c).wait_recv()
                for k in range(2):
                    b = (o_end, o_mid)[k]
                    own[l, g, c, b] = (own[l, g, c, b].astype(F32) + cmb[l, g, c, b - lo].astype(F32)).astype(BF16)
                    to_far(l, g, c, k).start()

        def finish(l, g, c):
            all_of(fin.at[l, g, c], rs_s, fn_r.at[l, g, c]).wait_recv()
            return (own[l, g, c, me].astype(F32) + fin[l, g, c, 0].astype(F32) + fin[l, g, c, 1].astype(F32)).astype(BF16)

        def x_phase(l, g):
            hrow = pl.ds(g * hb, hb)
            p_part = jnp.zeros((hb, rank + 2 * n_state), F32)
            for c in range(n_c):
                cols = pl.ds(c * chunk, chunk)
                x_new = finish(l, g, c)
                xi[l, hrow, cols] = x_new
                val = x_new.astype(F32) * cw[l, 3:4, cols] + cb[l : l + 1, cols]
                for k in range(3):
                    val = val + cs[l, k, hrow, cols].astype(F32) * cw[l, k : k + 1, cols]
                x_act = (val * jax.nn.sigmoid(val)).astype(BF16)
                xc[g, :, cols] = x_act.astype(F32)
                p_part = p_part + lax.dot_general(x_act, wx[l, :, cols], (((1,), (1,)), ((), ())), preferred_element_type=F32)
            pown[l, g] = p_part.astype(BF16)
            for j in range(1, n_ty):
                p_copy(l, g, j).start()

        def d_phase(l, g):
            p_sum = pown[l, g].astype(F32)
            all_of(pin.at[l, g], p_s, p_r.at[l, g]).wait_recv()
            for j in range(n_ty - 1):
                p_sum = p_sum + pin[l, g, j].astype(F32)
            dt_low = p_sum[:, :rank]
            dt_low = (dt_low * lax.rsqrt(jnp.mean(dt_low * dt_low, axis=-1, keepdims=True) + INNER_EPS)).astype(BF16)
            for i in range(2):
                mat = p_sum[:, rank + i * n_state : rank + (i + 1) * n_state]
                mat_t = (mat * lax.rsqrt(jnp.mean(mat * mat, axis=-1, keepdims=True) + INNER_EPS)).T
                for b in range(hb):
                    bc[g, i, b] = jnp.broadcast_to(mat_t[:, b : b + 1], (n_state, 128))
            dl[g] = dt_low

        def d_chunk(l, g, c):
            cols = pl.ds(c * chunk, chunk)
            dt_low = dl[g]
            raw = dot(dt_low, wdt[l, :, cols]) + db[l : l + 1, cols]
            delta = jnp.maximum(raw, 0.0) + jnp.log1p(jnp.exp(-jnp.abs(raw)))
            dt[:, cols] = delta
            dx[:, cols] = delta * xc[g, :, cols]
            neg_a = al[l, :, cols]

            def row_step(b, carry):
                row = pl.ds(b, 1)
                b_row = jnp.concatenate([bc[g, 0, b]] * (chunk // 128), axis=1)
                c_row = jnp.concatenate([bc[g, 1, b]] * (chunk // 128), axis=1)
                at = g * hb + b
                s_new = jnp.exp2(dt[row, cols] * neg_a) * ss[l, at, :, cols] + dx[row, cols] * b_row
                ss[l, at, :, cols] = s_new
                sv[g, row, cols] = jnp.sum(s_new * c_row, axis=0, keepdims=True)
                return carry

            lax.fori_loop(0, hb, row_step, 0, unroll=4)

        def y_phase(l, g, c):
            cols = pl.ds(c * chunk, chunk)
            z_new = finish(l, g, n_c + c).astype(F32)
            y = (sv[g, :, cols] + ds[l : l + 1, cols] * xc[g, :, cols]) * (z_new * jax.nn.sigmoid(z_new))
            yall[l, g, c, me] = y.astype(BF16)

            @pl.when(mid == 0)
            def _():
                ag_copy(l, g, c, me, 0, o_mid).start()

            @pl.when(mid == 1)
            def _():
                ag_copy(l, g, c, me, 1, o_end).start()
                ag_copy(l, g, c, me, 1, o_mid).start()

        def y_mate(l, g):
            for c in range(n_c):
                ag_copy(l, g, c, me, 1, mate).start()

        def gather(l, g, c):
            @pl.when(mid == 1)
            def _():
                ag_copy(l, g, c, o_end, 0, mate).wait_recv()
                ag_copy(l, g, c, o_end, 0, mate).start()

        def w_phase(l, g, c):
            @pl.when(mid == 0)
            def _():
                ag_copy(l, g, c, o_end, 0, mate).wait_recv()
            all_of(yall.at[l, g, c, pl.ds(0, 2)], ag_s, ag_r.at[l, g, c, 1]).wait_recv()
            y_all = yall[l, g, c].reshape(rg, chunk)
            for q in range(n_q):
                qc = pl.ds(q * qw, qw)
                out = dot(y_all, wout[l, pl.ds(c * chunk, chunk), qc])
                acc[g, :, qc] = out if c == 0 else acc[g, :, qc] + out
                if c == n_c - 1:
                    so[0, l, g, q] = acc[g, other, qc].astype(BF16)
                    s_copy(0, l, g, q).start()

        def sum_1(l, g):
            for q in range(n_q):
                s_copy(0, l, g, q).wait_recv()
                so[1, l, g, q] = (acc[g, mine, pl.ds(q * qw, qw)] + si[0, l, g, q].astype(F32)).astype(BF16)
                s_copy(1, l, g, q).start()

        def sum_2(l, g):
            for q in range(n_q):
                qc = pl.ds(q * qw, qw)
                s_copy(1, l, g, q).wait_recv()
                tot = (so[1, l, g, q].astype(F32) + si[1, l, g, q].astype(F32)).astype(BF16)
                so[2, l, g, q] = tot
                s_copy(2, l, g, q).start()
                r[g, mine, qc] += tot.astype(F32)

        def sum_3(l, g):
            for q in range(n_q):
                s_copy(2, l, g, q).wait_recv()
                r[g, other, pl.ds(q * qw, qw)] += si[2, l, g, q].astype(F32)

        ph = dict(
            stat=stat, head=head, norm=norm, out=out, send=send, c=combine, x=x_phase, d=d_phase, dc=d_chunk,
            y=y_phase, ym=y_mate, g=gather, w=w_phase, s1=sum_1, s2=sum_2, s3=sum_3,
        )

        def run(name, *args):
            with jax.named_scope(name + "_" + "_".join(map(str, args))):
                ph[name](*args)

        def proj(l, g, c, early=False):
            with jax.named_scope(f"proj_{l}_{g}_{c}"):
                project(l, g, c, early)
            if not early:
                send(l, g, c)

        groups, A, B = range(n_g), 0, 1
        for g in groups:
            start(*[("r", g, b) for b in range(n_tx)])
        start("nw")
        for k in range(1, n_tx):
            pl.semaphore_signal(barrier, 1, device_id=tx_of(lax.rem(me + k, n_tx)), device_id_type=MESH)
            pl.semaphore_signal(barrier, 1, device_id=(dp, lax.rem(me + k, n_tx), partner_ty), device_id_type=MESH)
        for k in range(1, n_ty):
            pl.semaphore_signal(barrier, 1, device_id=ty_of(lax.rem(ty + k, n_ty)), device_id_type=MESH)
        for g in groups:
            wait(*[("r", g, b) for b in range(n_tx)])
        wait("nw")
        start(*[("win", 0, t) for t in range(n_w)])
        pl.semaphore_wait(barrier, 2 * (n_tx - 1) + n_ty - 1)
        for g in groups:
            run("stat", 0, g)
        start("cw", "cb", "db", "al", "ds", "cs", ("wx", 0), ("wdt", 0), ("ss", 0), ("wout", 0))
        def each(name, l, g, *cs):
            for c in cs:
                run(name, l, g, c)

        X, Z = range(n_c), range(n_c, 2 * n_c)
        head2, tail2, l0, l1 = X[:2], X[2:], 0, n_layer - 1
        early = n_w // 2

        run("head", l0, A)
        wait(*[("win", l0, t) for t in range(early)])
        for c in head2:
            proj(l0, A, c, True)
        run("norm", l0, A)
        each("out", l0, A, *head2)
        wait(*[("win", l0, t) for t in range(early, n_w)])
        for c in tail2:
            proj(l0, A, c)
        each("send", l0, A, *Z)
        run("head", l0, B)
        run("norm", l0, B)
        for c in X[:-1]:
            run("c", l0, A, c)
            proj(l0, B, c)
        start(*[("win", l1, t) for t in range(n_w)])
        start(("wx", l1), ("wdt", l1), ("ss", l1), ("wout", l1))
        wait("cw", "cb", "db", "al", "ds", "cs", ("wx", l0))
        al[...] = -jnp.exp(al[...]) * LOG2E
        run("c", l0, A, X[-1])
        proj(l0, B, X[-1])
        run("send", l0, B, Z[0])
        each("c", l0, A, *Z[:2])
        run("x", l0, A)
        each("c", l0, A, *Z[2:])
        each("c", l0, B, *head2)
        wait(("wdt", l0), ("ss", l0))
        run("d", l0, A)
        each("dc", l0, A, *head2)
        run("c", l0, B, X[2])
        each("dc", l0, A, *tail2)
        run("c", l0, B, X[-1])
        each("y", l0, A, *X)
        run("ym", l0, A)
        each("send", l0, B, *Z[1:])
        run("c", l0, B, Z[0])
        each("g", l0, A, *head2)
        run("x", l0, B)
        each("g", l0, A, *tail2)
        each("c", l0, B, *Z[1:3])
        wait(("wout", l0))
        each("w", l0, A, *X)
        run("c", l0, B, Z[-1])
        run("s1", l0, A)
        run("d", l0, B)
        each("dc", l0, B, *X)
        run("s2", l0, A)
        run("stat", l1, A)
        each("y", l0, B, *X)
        run("ym", l0, B)
        run("s3", l0, A)
        wait(*[("win", l1, t) for t in range(n_w)])
        run("head", l1, A)
        for c in head2:
            proj(l1, A, c, True)
        run("norm", l1, A)
        each("out", l1, A, *head2)
        each("g", l0, B, *X)
        for c in tail2:
            proj(l1, A, c)
        each("w", l0, B, *X)
        each("c", l1, A, *head2)
        run("s1", l0, B)
        each("c", l1, A, *tail2)
        run("s2", l0, B)
        run("stat", l1, B)
        each("send", l1, A, *Z)
        run("s3", l0, B)
        run("head", l1, B)
        for c in head2:
            proj(l1, B, c, True)
        wait(("wx", l1))
        run("x", l1, A)
        run("norm", l1, B)
        each("out", l1, B, *head2)
        proj(l1, B, X[2])
        each("c", l1, A, *Z[:2])
        proj(l1, B, X[-1])
        each("c", l1, A, *Z[2:])
        wait(("wdt", l1), ("ss", l1))
        run("d", l1, A)
        each("send", l1, B, *Z[:2])
        each("dc", l1, A, *head2)
        run("c", l1, B, X[0])
        each("send", l1, B, *Z[2:])
        each("dc", l1, A, *tail2)
        each("c", l1, B, *X[1:])
        each("y", l1, A, *X)
        run("ym", l1, A)
        each("c", l1, B, *Z[:2])
        run("x", l1, B)
        each("c", l1, B, *Z[2:])
        each("g", l1, A, *X)
        run("d", l1, B)
        for c in X:
            run("dc", l1, B, c)
            run("y", l1, B, c)
        run("ym", l1, B)
        wait(("wout", l1))
        each("w", l1, A, *X)
        each("g", l1, B, *head2)
        run("s1", l1, A)
        for c in head2:
            run("w", l1, B, c)
            run("g", l1, B, c + 2)
        each("w", l1, B, *tail2)
        run("s2", l1, A)
        run("s1", l1, B)
        run("s3", l1, A)
        run("s2", l1, B)
        run("s3", l1, B)

        with jax.named_scope("end"):
            all_of(own.at[:, :, :, pl.ds(0, 3)], rs_s, fn_r.at[0, 0, 0]).wait_send()
            all_of(sti, st_s, fn_r.at[0, 0, 0]).wait_send()
            all_of(pin, p_s, fn_r.at[0, 0, 0]).wait_send()
            all_of(so, s_s, fn_r.at[0, 0, 0]).wait_send()

            @pl.when(mid == 0)
            def _():
                all_of(yall.at[:, :, :, pl.ds(0, 2)], ag_s, fn_r.at[0, 0, 0]).wait_send()

            @pl.when(mid == 1)
            def _():
                all_of(yall, ag_s, fn_r.at[0, 0, 0]).wait_send()

    def dma(*s):
        return pltpu.SemaphoreType.DMA(s) if s else pltpu.SemaphoreType.DMA

    def vm(t, *s):
        return pltpu.VMEM(s, t)

    nl, p_w = n_layer, rank + 2 * n_state
    scratch = [
        vm(F32, nl, d_loc), vm(BF16, nl, n_w, d_loc, 2, 128), vm(F32, nl, 4, chan), vm(F32, nl, chan),
        vm(BF16, nl, p_w, chan), vm(BF16, nl, rank, chan), vm(F32, nl, chan), vm(F32, nl, n_state, chan), vm(F32, nl, chan),
        vm(BF16, nl, chan, d_loc),
        vm(BF16, n_g, 2 * rg, 2 * d_loc), vm(BF16, nl, n_g, 2 * n_c, n_tx, hb, chunk),
        vm(BF16, nl, n_g, 2 * n_c, 2, hb, chunk), vm(BF16, nl, n_g, 2 * n_c, 2, hb, chunk),
        vm(F32, n_g, hb, chan), vm(F32, hb, chan), vm(F32, hb, chan), vm(F32, n_g, hb, chan),
        vm(F32, n_g, 2, hb, n_state, 128), vm(BF16, n_g, hb, rank), vm(BF16, nl, n_g, hb, p_w), vm(BF16, nl, n_g, n_ty - 1, hb, p_w),
        vm(BF16, nl, n_g, n_c, n_tx, hb, chunk), vm(F32, n_g, rg, d_loc),
        vm(BF16, 3, nl, n_g, n_q, half, qw), vm(BF16, 3, nl, n_g, n_q, half, qw),
        vm(F32, nl, n_g, 8, half), vm(F32, nl, n_g, 2 * n_tx - 1, 8, half), vm(F32, rg, 128), vm(F32, n_g, rg, 128), vm(F32, 2, 2 * rg, chunk),
        dma(7 + 4 * nl), dma(n_g, n_tx), dma(nl, n_w),
        dma(), dma(nl, n_g, 2 * n_c), dma(nl, n_g, 2 * n_c),
        dma(), dma(nl, n_g), dma(), dma(nl, n_g, n_c, 2),
        dma(), dma(nl, n_g, 3, n_q), dma(), dma(nl, n_g),
    ]
    outs = (vm(F32, n_g, rg, d_loc), vm(BF16, nl, blk, chan), vm(BF16, nl, 3, blk, chan), vm(F32, nl, blk, n_state, chan))
    return kernel, outs, scratch


def store_kernel(r, xi, cs, ss, r_out, conv_out, ssm_out, sem):
    n_g, rg, _ = r.shape
    nl, blk = ss.shape[:2]
    hb = blk // n_g
    pairs = []
    for l in range(nl):
        for i in range(0, blk, 8):
            pairs.append((ss.at[l, pl.ds(i, 8)], ssm_out.at[l, pl.ds(i, 8)]))
    for l in range(nl):
        pairs.append((cs.at[l, pl.ds(1, 2)], conv_out.at[l, pl.ds(0, 2)]))
        pairs.append((xi.at[l], conv_out.at[l, 2]))
    for g in range(n_g):
        for b in range(rg // hb):
            pairs.append((r.at[g, pl.ds(b * hb, hb)], r_out.at[pl.ds(b * blk + g * hb, hb)]))
    copies = [pltpu.make_async_copy(src, dst, sem.at[i]) for i, (src, dst) in enumerate(pairs)]
    for cp in copies:
        cp.start()
    for cp in copies:
        cp.wait()


def solution(mesh):
    n_tx, n_ty = mesh.shape["tx"], mesh.shape["ty"]

    def local_step(residual, norm_w, w_in, conv_w, conv_b, w_x, w_dt, dt_bias, a_log, d_skip, w_out, conv_state, ssm_state):
        rows, d_loc = residual.shape
        n_layer, _, _, chan = w_in.shape
        rank, n_state = w_dt.shape[1], a_log.shape[-1]
        blk = rows // n_tx
        kernel, outs, scratch = make_kernel(n_layer, n_tx, n_ty, rows, d_loc, chan, rank, n_state, 512, 2, 2)
        parts = pl.pallas_call(
            kernel,
            out_shape=outs,
            in_specs=[ANY] * 13,
            out_specs=(VMEM,) * 4,
            scratch_shapes=scratch,
            compiler_params=pltpu.CompilerParams(collective_id=0, has_side_effects=True, vmem_limit_bytes=67043328 - 11 * 2**20),
            name="mixer",
        )(
            residual, norm_w, w_in, conv_w.transpose(0, 2, 1), conv_b, w_x.transpose(0, 2, 1), w_dt, dt_bias,
            a_log.transpose(0, 2, 1), d_skip, w_out, conv_state.transpose(0, 3, 1, 2), ssm_state.transpose(0, 1, 3, 2),
        )
        r_out, conv_out, ssm_out = pl.pallas_call(
            store_kernel,
            out_shape=(
                jax.ShapeDtypeStruct((rows, d_loc), F32),
                jax.ShapeDtypeStruct((n_layer, 3, blk, chan), BF16),
                jax.ShapeDtypeStruct((n_layer, blk, n_state, chan), F32),
            ),
            in_specs=[VMEM] * 4,
            out_specs=(ANY,) * 3,
            scratch_shapes=[pltpu.SemaphoreType.DMA((64,))],
            compiler_params=pltpu.CompilerParams(vmem_limit_bytes=12 * 2**20),
            name="store",
        )(*parts)
        return r_out, conv_out.transpose(0, 2, 3, 1), ssm_out.transpose(0, 1, 3, 2)

    cache_spec = P(None, ("dp", "tx"), "ty", None)
    in_specs = (P("dp", "tx"), P(None, "tx"), P(None, "tx", None, "ty"), P(None, "ty", None), P(None, "ty"), P(None, "ty", None), P(None, None, "ty"), P(None, "ty"), P(None, "ty", None), P(None, "ty"), P(None, "ty", "tx"), cache_spec, cache_spec)
    out_specs = (P("dp", "tx"), cache_spec, cache_spec)
    return jax.shard_map(local_step, mesh=mesh, in_specs=in_specs, out_specs=out_specs, check_vma=False)
```

```python
import jax
import jax.numpy as jnp
from jax import lax
from jax.experimental import pallas as pl
from jax.experimental.pallas import tpu as pltpu
from jax.sharding import PartitionSpec as P

NORM_EPS = 1e-5
INNER_EPS = 1e-6
LOG2E = 1.4426950408889634
BF16, F32 = jnp.bfloat16, jnp.float32
MESH = pl.DeviceIdType.MESH
ANY = pl.BlockSpec(memory_space=pl.ANY)
VMEM = pl.BlockSpec(memory_space=pltpu.VMEM)


def dot(a, b):
    return jnp.dot(a, b, preferred_element_type=F32)


def make_kernel(n_layer, n_tx, n_ty, rows, d_loc, chan, rank, n_state, chunk, n_g, n_q):
    blk = rows // n_tx
    hb = blk // n_g
    rg = n_tx * hb
    half = rg // 2
    n_c = chan // chunk
    d_model = d_loc * n_tx
    qw = d_loc // n_q
    n_w = chan // 128

    def kernel(
        r_hbm, nw_hbm, win_hbm, cw_hbm, cb_hbm, wx_hbm, wdt_hbm, db_hbm, al_hbm, ds_hbm, wout_hbm, cs_hbm, ss_hbm,
        r, xi, cs, ss,
        nw, win, cw, cb, wx, wdt, db, al, ds, wout,
        hx, own, cmb, fin, xc, dt, dx, sv, bc, dl, pown, pin, yall, acc, so, si, sto, sti, sc, sl, pf,
        ld_sem, r_sem, win_sem, rs_s, cm_r, fn_r, p_s, p_r, ag_s, ag_r, s_s, s_r, st_s, st_r,
    ):
        dp, me, ty = lax.axis_index("dp"), lax.axis_index("tx"), lax.axis_index("ty")
        core = lax.rem(ty, 2)
        mate = me + 1 - 2 * lax.rem(me, 2)
        mid = (me * (3 - me)) // 2
        o_end = 3 - me + mid * (me - mate)
        o_mid = 3 - mate + mid * (mate - me)
        lo = 2 * (1 - me // 2)
        barrier = pltpu.get_barrier_semaphore()

        def tx_of(k):
            return (dp, k, ty)

        def ty_of(k):
            return (dp, me, k)

        def remote(src, dst, ssem, rsem, dev):
            return pltpu.make_async_remote_copy(src_ref=src, dst_ref=dst, send_sem=ssem, recv_sem=rsem, device_id=dev, device_id_type=MESH)

        loads = {}
        for g in range(n_g):
            for b in range(n_tx):
                loads["r", g, b] = pltpu.make_async_copy(r_hbm.at[pl.ds(b * blk + g * hb, hb)], r.at[g, pl.ds(b * hb, hb)], r_sem.at[g, b])
        names = dict(nw=(nw_hbm, nw), cw=(cw_hbm, cw), cb=(cb_hbm, cb), db=(db_hbm, db), al=(al_hbm, al), ds=(ds_hbm, ds), cs=(cs_hbm, cs))
        for k, key in enumerate(names):
            loads[key] = pltpu.make_async_copy(names[key][0], names[key][1], ld_sem.at[k])
        for l in range(n_layer):
            for k, (key, src, dst) in enumerate((("wx", wx_hbm, wx), ("wdt", wdt_hbm, wdt), ("wout", wout_hbm, wout), ("ss", ss_hbm, ss))):
                loads[key, l] = pltpu.make_async_copy(src.at[l], dst.at[l], ld_sem.at[len(names) + 4 * l + k])
            for t in range(n_w):
                loads["win", l, t] = pltpu.make_async_copy(win_hbm.at[l, :, :, pl.ds(t * 128, 128)], win.at[l, t], win_sem.at[l, t])

        def start(*keys):
            for key in keys:
                loads[key].start()

        def wait(*keys):
            for key in keys:
                loads[key].wait()

        partner_ty = ty + 1 - 2 * core
        partner = ty_of(partner_ty)
        across = ty_of(lax.rem(ty + 2, n_ty))
        mine = pl.ds(pl.multiple_of(core * half, half), half)
        other = pl.ds(pl.multiple_of((1 - core) * half, half), half)

        def stat_copy(l, g, j, rel):
            dev = (dp, lax.rem(me + j, n_tx), partner_ty if rel else ty)
            return remote(sto.at[l, g], sti.at[l, g, 2 * j + rel - 1], st_s, st_r.at[l, g], dev)

        def to_mate(l, g, c):
            return remote(own.at[l, g, c, mate], fin.at[l, g, c, 0], rs_s, fn_r.at[l, g, c], tx_of(mate))

        def to_mid(l, g, c):
            return remote(own.at[l, g, c, pl.ds(lo, 2)], cmb.at[l, g, c], rs_s, cm_r.at[l, g, c], tx_of(mate))

        def to_far(l, g, c, k):
            b = (o_end, o_mid)[k]
            return remote(own.at[l, g, c, b], fin.at[l, g, c, 1], rs_s, fn_r.at[l, g, c], tx_of(b))

        def p_copy(l, g, j):
            return remote(pown.at[l, g], pin.at[l, g, j - 1], p_s, p_r.at[l, g], ty_of(lax.rem(ty + j, n_ty)))

        def ag_copy(l, g, c, b, k, dev):
            return remote(yall.at[l, g, c, b], yall.at[l, g, c, b], ag_s, ag_r.at[l, g, c, k], tx_of(dev))

        def s_copy(i, l, g, q):
            return remote(so.at[i, l, g, q], si.at[i, l, g, q], s_s, s_r.at[l, g, i, q], across if i == 1 else partner)

        def all_of(ref, ssem, rsem):
            return remote(ref, ref, ssem, rsem, partner)

        def stat(l, g):
            part = r[g, mine, :]
            sq = jnp.sum(part * part, axis=-1, keepdims=True)
            sto[l, g] = jnp.broadcast_to(sq, (half, 128)).T[0:8, :]
            for j in range(n_tx - 1, -1, -1):
                for rel in range(2):
                    if j or rel:
                        stat_copy(l, g, j, rel).start()

        def head(l, g):
            for b in range(2):
                at = pl.ds(b * half, half)
                part = r[g, at, :]
                sq = jnp.sum(part * part, axis=-1, keepdims=True)
                sl[g, at, :] = lax.rsqrt(jnp.broadcast_to(sq, (half, 128)) / d_model + NORM_EPS)
            scale = sl[g]
            row_i = lax.broadcasted_iota(jnp.int32, (128, 256), 0)
            col_i = lax.broadcasted_iota(jnp.int32, (128, 256), 1)
            pick = [(col_i == 2 * row_i + k).astype(F32).astype(BF16) for k in range(2)]
            for j in range(d_loc // 128):
                cols = pl.ds(j * 128, 128)
                h = (r[g, :, cols] * scale * nw[l : l + 1, cols]).astype(BF16)
                for k in range(2):
                    hx[g, k * rg : (k + 1) * rg, pl.ds(j * 256, 256)] = dot(h, pick[k]).astype(BF16)

        def norm(l, g):
            all_of(sti.at[l, g], st_s, st_r.at[l, g]).wait_recv()
            for rel, at in enumerate((mine, other)):
                tot = sto[l, g] if rel == 0 else sti[l, g, 0]
                for j in range(1, n_tx):
                    tot = tot + sti[l, g, 2 * j + rel - 1]
                sc[at, :] = lax.rsqrt(jnp.broadcast_to(tot[0:1, :], (128, half)).T / d_model + NORM_EPS)
            sl[g] = jnp.where(sl[g] > 0.0, sc[...] / sl[g], 0.0)

        def project(l, g, c, early):
            for t in range(0, chunk // 128, 2):
                tile = c * (chunk // 128) + t
                w = jnp.concatenate([win.at[l, tile + i].reshape(2 * d_loc, 128)[...] for i in range(2)], axis=1)
                part = dot(hx[g], w)
                if early:
                    pf[c, :, pl.ds(t * 128, 256)] = part
                else:
                    scaled(l, g, c, t, part)

        def scaled(l, g, c, t, part):
            ratio = jnp.concatenate([sl[g], sl[g]], axis=1)
            for k in range(2):
                piece = (part[k * rg : (k + 1) * rg, :] * ratio).astype(BF16)
                for b in range(n_tx):
                    own[l, g, k * n_c + c, b, :, pl.ds(t * 128, 256)] = piece[b * hb : (b + 1) * hb, :]

        def out(l, g, c):
            for t in range(0, chunk // 128, 2):
                scaled(l, g, c, t, pf[c, :, pl.ds(t * 128, 256)])
            send(l, g, c)

        def send(l, g, c):
            @pl.when(mid == 0)
            def _():
                to_mid(l, g, c).start()
            to_mate(l, g, c).start()

        def combine(l, g, c):
            @pl.when(mid == 1)
            def _():
                to_mid(l, g, c).wait_recv()
                for k in range(2):
                    b = (o_end, o_mid)[k]
                    own[l, g, c, b] = (own[l, g, c, b].astype(F32) + cmb[l, g, c, b - lo].astype(F32)).astype(BF16)
                    to_far(l, g, c, k).start()

        def finish(l, g, c):
            all_of(fin.at[l, g, c], rs_s, fn_r.at[l, g, c]).wait_recv()
            return (own[l, g, c, me].astype(F32) + fin[l, g, c, 0].astype(F32) + fin[l, g, c, 1].astype(F32)).astype(BF16)

        def x_phase(l, g):
            hrow = pl.ds(g * hb, hb)
            p_part = jnp.zeros((hb, rank + 2 * n_state), F32)
            for c in range(n_c):
                cols = pl.ds(c * chunk, chunk)
                x_new = finish(l, g, c)
                xi[l, hrow, cols] = x_new
                val = x_new.astype(F32) * cw[l, 3:4, cols] + cb[l : l + 1, cols]
                for k in range(3):
                    val = val + cs[l, k, hrow, cols].astype(F32) * cw[l, k : k + 1, cols]
                x_act = (val * jax.nn.sigmoid(val)).astype(BF16)
                xc[g, :, cols] = x_act.astype(F32)
                p_part = p_part + lax.dot_general(x_act, wx[l, :, cols], (((1,), (1,)), ((), ())), preferred_element_type=F32)
            pown[l, g] = p_part.astype(BF16)
            for j in range(1, n_ty):
                p_copy(l, g, j).start()

        def d_phase(l, g):
            p_sum = pown[l, g].astype(F32)
            all_of(pin.at[l, g], p_s, p_r.at[l, g]).wait_recv()
            for j in range(n_ty - 1):
                p_sum = p_sum + pin[l, g, j].astype(F32)
            dt_low = p_sum[:, :rank]
            dt_low = (dt_low * lax.rsqrt(jnp.mean(dt_low * dt_low, axis=-1, keepdims=True) + INNER_EPS)).astype(BF16)
            for i in range(2):
                mat = p_sum[:, rank + i * n_state : rank + (i + 1) * n_state]
                mat_t = (mat * lax.rsqrt(jnp.mean(mat * mat, axis=-1, keepdims=True) + INNER_EPS)).T
                for b in range(hb):
                    bc[g, i, b] = jnp.broadcast_to(mat_t[:, b : b + 1], (n_state, 128))
            dl[g] = dt_low

        def d_chunk(l, g, c):
            cols = pl.ds(c * chunk, chunk)
            dt_low = dl[g]
            raw = dot(dt_low, wdt[l, :, cols]) + db[l : l + 1, cols]
            delta = jnp.maximum(raw, 0.0) + jnp.log1p(jnp.exp(-jnp.abs(raw)))
            dt[:, cols] = delta
            dx[:, cols] = delta * xc[g, :, cols]
            neg_a = al[l, :, cols]

            def row_step(b, carry):
                row = pl.ds(b, 1)
                b_row = jnp.concatenate([bc[g, 0, b]] * (chunk // 128), axis=1)
                c_row = jnp.concatenate([bc[g, 1, b]] * (chunk // 128), axis=1)
                at = g * hb + b
                s_new = jnp.exp2(dt[row, cols] * neg_a) * ss[l, at, :, cols] + dx[row, cols] * b_row
                ss[l, at, :, cols] = s_new
                sv[g, row, cols] = jnp.sum(s_new * c_row, axis=0, keepdims=True)
                return carry

            lax.fori_loop(0, hb, row_step, 0, unroll=4)

        def y_phase(l, g, c):
            cols = pl.ds(c * chunk, chunk)
            z_new = finish(l, g, n_c + c).astype(F32)
            y = (sv[g, :, cols] + ds[l : l + 1, cols] * xc[g, :, cols]) * (z_new * jax.nn.sigmoid(z_new))
            yall[l, g, c, me] = y.astype(BF16)

            @pl.when(mid == 0)
            def _():
                ag_copy(l, g, c, me, 0, o_mid).start()

            @pl.when(mid == 1)
            def _():
                ag_copy(l, g, c, me, 1, o_end).start()
                ag_copy(l, g, c, me, 1, o_mid).start()

        def y_mate(l, g):
            for c in range(n_c):
                ag_copy(l, g, c, me, 1, mate).start()

        def gather(l, g, c):
            @pl.when(mid == 1)
            def _():
                ag_copy(l, g, c, o_end, 0, mate).wait_recv()
                ag_copy(l, g, c, o_end, 0, mate).start()

        def w_phase(l, g, c):
            @pl.when(mid == 0)
            def _():
                ag_copy(l, g, c, o_end, 0, mate).wait_recv()
            all_of(yall.at[l, g, c, pl.ds(0, 2)], ag_s, ag_r.at[l, g, c, 1]).wait_recv()
            y_all = yall[l, g, c].reshape(rg, chunk)
            for q in range(n_q):
                qc = pl.ds(q * qw, qw)
                out = dot(y_all, wout[l, pl.ds(c * chunk, chunk), qc])
                acc[g, :, qc] = out if c == 0 else acc[g, :, qc] + out
                if c == n_c - 1:
                    so[0, l, g, q] = acc[g, other, qc].astype(BF16)
                    s_copy(0, l, g, q).start()

        def sum_1(l, g):
            for q in range(n_q):
                s_copy(0, l, g, q).wait_recv()
                so[1, l, g, q] = (acc[g, mine, pl.ds(q * qw, qw)] + si[0, l, g, q].astype(F32)).astype(BF16)
                s_copy(1, l, g, q).start()

        def sum_2(l, g):
            for q in range(n_q):
                qc = pl.ds(q * qw, qw)
                s_copy(1, l, g, q).wait_recv()
                tot = (so[1, l, g, q].astype(F32) + si[1, l, g, q].astype(F32)).astype(BF16)
                so[2, l, g, q] = tot
                s_copy(2, l, g, q).start()
                r[g, mine, qc] += tot.astype(F32)

        def sum_3(l, g):
            for q in range(n_q):
                s_copy(2, l, g, q).wait_recv()
                r[g, other, pl.ds(q * qw, qw)] += si[2, l, g, q].astype(F32)

        ph = dict(
            stat=stat, head=head, norm=norm, out=out, send=send, c=combine, x=x_phase, d=d_phase, dc=d_chunk,
            y=y_phase, ym=y_mate, g=gather, w=w_phase, s1=sum_1, s2=sum_2, s3=sum_3,
        )

        def run(name, *args):
            with jax.named_scope(name + "_" + "_".join(map(str, args))):
                ph[name](*args)

        def proj(l, g, c, early=False):
            with jax.named_scope(f"proj_{l}_{g}_{c}"):
                project(l, g, c, early)
            if not early:
                send(l, g, c)

        groups, A, B = range(n_g), 0, 1
        for g in groups:
            start(*[("r", g, b) for b in range(n_tx)])
        start("nw")
        for k in range(1, n_tx):
            pl.semaphore_signal(barrier, 1, device_id=tx_of(lax.rem(me + k, n_tx)), device_id_type=MESH)
            pl.semaphore_signal(barrier, 1, device_id=(dp, lax.rem(me + k, n_tx), partner_ty), device_id_type=MESH)
        for k in range(1, n_ty):
            pl.semaphore_signal(barrier, 1, device_id=ty_of(lax.rem(ty + k, n_ty)), device_id_type=MESH)
        for g in groups:
            wait(*[("r", g, b) for b in range(n_tx)])
        wait("nw")
        start(*[("win", 0, t) for t in range(n_w)])
        pl.semaphore_wait(barrier, 2 * (n_tx - 1) + n_ty - 1)
        for g in groups:
            run("stat", 0, g)
        start("cw", "cb", "db", "al", "ds", "cs", ("wx", 0), ("wdt", 0), ("ss", 0), ("wout", 0))
        def each(name, l, g, *cs):
            for c in cs:
                run(name, l, g, c)

        X, Z = range(n_c), range(n_c, 2 * n_c)
        head2, tail2, l0, l1 = X[:2], X[2:], 0, n_layer - 1
        early = n_w // 2

        run("head", l0, A)
        wait(*[("win", l0, t) for t in range(early)])
        for c in head2:
            proj(l0, A, c, True)
        run("norm", l0, A)
        each("out", l0, A, *head2)
        wait(*[("win", l0, t) for t in range(early, n_w)])
        for c in tail2:
            proj(l0, A, c)
        each("send", l0, A, *Z)
        run("head", l0, B)
        run("norm", l0, B)
        for c in X[:-1]:
            run("c", l0, A, c)
            proj(l0, B, c)
        start(*[("win", l1, t) for t in range(n_w)])
        start(("wx", l1), ("wdt", l1), ("ss", l1), ("wout", l1))
        wait("cw", "cb", "db", "al", "ds", "cs", ("wx", l0))
        al[...] = -jnp.exp(al[...]) * LOG2E
        run("c", l0, A, X[-1])
        proj(l0, B, X[-1])
        run("send", l0, B, Z[0])
        each("c", l0, A, *Z[:2])
        run("x", l0, A)
        each("c", l0, A, *Z[2:])
        each("c", l0, B, *head2)
        wait(("wdt", l0), ("ss", l0))
        run("d", l0, A)
        each("dc", l0, A, *head2)
        run("c", l0, B, X[2])
        each("dc", l0, A, *tail2)
        run("c", l0, B, X[-1])
        each("y", l0, A, *X)
        run("ym", l0, A)
        each("send", l0, B, *Z[1:])
        run("c", l0, B, Z[0])
        each("g", l0, A, *head2)
        run("x", l0, B)
        each("g", l0, A, *tail2)
        each("c", l0, B, *Z[1:3])
        wait(("wout", l0))
        each("w", l0, A, *X)
        run("c", l0, B, Z[-1])
        run("s1", l0, A)
        run("d", l0, B)
        each("dc", l0, B, *X)
        run("s2", l0, A)
        run("stat", l1, A)
        each("y", l0, B, *X)
        run("ym", l0, B)
        run("s3", l0, A)
        wait(*[("win", l1, t) for t in range(n_w)])
        run("head", l1, A)
        for c in head2:
            proj(l1, A, c, True)
        run("norm", l1, A)
        each("out", l1, A, *head2)
        each("g", l0, B, *X)
        for c in tail2:
            proj(l1, A, c)
        each("w", l0, B, *X)
        each("c", l1, A, *head2)
        run("s1", l0, B)
        each("c", l1, A, *tail2)
        run("s2", l0, B)
        run("stat", l1, B)
        each("send", l1, A, *Z)
        run("s3", l0, B)
        run("head", l1, B)
        for c in head2:
            proj(l1, B, c, True)
        wait(("wx", l1))
        run("x", l1, A)
        run("norm", l1, B)
        each("out", l1, B, *head2)
        proj(l1, B, X[2])
        each("c", l1, A, *Z[:2])
        proj(l1, B, X[-1])
        each("c", l1, A, *Z[2:])
        wait(("wdt", l1), ("ss", l1))
        run("d", l1, A)
        each("send", l1, B, *Z[:2])
        each("dc", l1, A, *head2)
        run("c", l1, B, X[0])
        each("send", l1, B, *Z[2:])
        each("dc", l1, A, *tail2)
        each("c", l1, B, *X[1:])
        each("y", l1, A, *X)
        run("ym", l1, A)
        each("c", l1, B, *Z[:2])
        run("x", l1, B)
        each("c", l1, B, *Z[2:])
        each("g", l1, A, *X)
        run("d", l1, B)
        for c in X:
            run("dc", l1, B, c)
            run("y", l1, B, c)
        run("ym", l1, B)
        wait(("wout", l1))
        each("w", l1, A, *X)
        each("g", l1, B, *head2)
        run("s1", l1, A)
        for c in head2:
            run("w", l1, B, c)
            run("g", l1, B, c + 2)
        each("w", l1, B, *tail2)
        run("s2", l1, A)
        run("s1", l1, B)
        run("s3", l1, A)
        run("s2", l1, B)
        run("s3", l1, B)

        with jax.named_scope("end"):
            all_of(own.at[:, :, :, pl.ds(0, 3)], rs_s, fn_r.at[0, 0, 0]).wait_send()
            all_of(sti, st_s, fn_r.at[0, 0, 0]).wait_send()
            all_of(pin, p_s, fn_r.at[0, 0, 0]).wait_send()
            all_of(so, s_s, fn_r.at[0, 0, 0]).wait_send()

            @pl.when(mid == 0)
            def _():
                all_of(yall.at[:, :, :, pl.ds(0, 2)], ag_s, fn_r.at[0, 0, 0]).wait_send()

            @pl.when(mid == 1)
            def _():
                all_of(yall, ag_s, fn_r.at[0, 0, 0]).wait_send()

    def dma(*s):
        return pltpu.SemaphoreType.DMA(s) if s else pltpu.SemaphoreType.DMA

    def vm(t, *s):
        return pltpu.VMEM(s, t)

    nl, p_w = n_layer, rank + 2 * n_state
    scratch = [
        vm(F32, nl, d_loc), vm(BF16, nl, n_w, d_loc, 2, 128), vm(F32, nl, 4, chan), vm(F32, nl, chan),
        vm(BF16, nl, p_w, chan), vm(BF16, nl, rank, chan), vm(F32, nl, chan), vm(F32, nl, n_state, chan), vm(F32, nl, chan),
        vm(BF16, nl, chan, d_loc),
        vm(BF16, n_g, 2 * rg, 2 * d_loc), vm(BF16, nl, n_g, 2 * n_c, n_tx, hb, chunk),
        vm(BF16, nl, n_g, 2 * n_c, 2, hb, chunk), vm(BF16, nl, n_g, 2 * n_c, 2, hb, chunk),
        vm(F32, n_g, hb, chan), vm(F32, hb, chan), vm(F32, hb, chan), vm(F32, n_g, hb, chan),
        vm(F32, n_g, 2, hb, n_state, 128), vm(BF16, n_g, hb, rank), vm(BF16, nl, n_g, hb, p_w), vm(BF16, nl, n_g, n_ty - 1, hb, p_w),
        vm(BF16, nl, n_g, n_c, n_tx, hb, chunk), vm(F32, n_g, rg, d_loc),
        vm(BF16, 3, nl, n_g, n_q, half, qw), vm(BF16, 3, nl, n_g, n_q, half, qw),
        vm(F32, nl, n_g, 8, half), vm(F32, nl, n_g, 2 * n_tx - 1, 8, half), vm(F32, rg, 128), vm(F32, n_g, rg, 128), vm(F32, 2, 2 * rg, chunk),
        dma(7 + 4 * nl), dma(n_g, n_tx), dma(nl, n_w),
        dma(), dma(nl, n_g, 2 * n_c), dma(nl, n_g, 2 * n_c),
        dma(), dma(nl, n_g), dma(), dma(nl, n_g, n_c, 2),
        dma(), dma(nl, n_g, 3, n_q), dma(), dma(nl, n_g),
    ]
    outs = (vm(F32, n_g, rg, d_loc), vm(BF16, nl, blk, chan), vm(BF16, nl, 3, blk, chan), vm(F32, nl, blk, n_state, chan))
    return kernel, outs, scratch


def store_kernel(r, xi, cs, ss, r_out, conv_out, ssm_out, sem):
    n_g, rg, _ = r.shape
    nl, blk = ss.shape[:2]
    hb = blk // n_g
    pairs = []
    for l in range(nl):
        for i in range(0, blk, 8):
            pairs.append((ss.at[l, pl.ds(i, 8)], ssm_out.at[l, pl.ds(i, 8)]))
    for l in range(nl):
        pairs.append((cs.at[l, pl.ds(1, 2)], conv_out.at[l, pl.ds(0, 2)]))
        pairs.append((xi.at[l], conv_out.at[l, 2]))
    for g in range(n_g):
        for b in range(rg // hb):
            pairs.append((r.at[g, pl.ds(b * hb, hb)], r_out.at[pl.ds(b * blk + g * hb, hb)]))
    copies = [pltpu.make_async_copy(src, dst, sem.at[i]) for i, (src, dst) in enumerate(pairs)]
    for cp in copies:
        cp.start()
    for cp in copies:
        cp.wait()


def solution(mesh):
    n_tx, n_ty = mesh.shape["tx"], mesh.shape["ty"]

    def local_step(residual, norm_w, w_in, conv_w, conv_b, w_x, w_dt, dt_bias, a_log, d_skip, w_out, conv_state, ssm_state):
        rows, d_loc = residual.shape
        n_layer, _, _, chan = w_in.shape
        rank, n_state = w_dt.shape[1], a_log.shape[-1]
        blk = rows // n_tx
        kernel, outs, scratch = make_kernel(n_layer, n_tx, n_ty, rows, d_loc, chan, rank, n_state, 512, 2, 4)
        parts = pl.pallas_call(
            kernel,
            out_shape=outs,
            in_specs=[ANY] * 13,
            out_specs=(VMEM,) * 4,
            scratch_shapes=scratch,
            compiler_params=pltpu.CompilerParams(collective_id=0, has_side_effects=True, vmem_limit_bytes=67043328 - 11 * 2**20),
            name="mixer",
        )(
            residual, norm_w, w_in, conv_w.transpose(0, 2, 1), conv_b, w_x.transpose(0, 2, 1), w_dt, dt_bias,
            a_log.transpose(0, 2, 1), d_skip, w_out, conv_state.transpose(0, 3, 1, 2), ssm_state.transpose(0, 1, 3, 2),
        )
        r_out, conv_out, ssm_out = pl.pallas_call(
            store_kernel,
            out_shape=(
                jax.ShapeDtypeStruct((rows, d_loc), F32),
                jax.ShapeDtypeStruct((n_layer, 3, blk, chan), BF16),
                jax.ShapeDtypeStruct((n_layer, blk, n_state, chan), F32),
            ),
            in_specs=[VMEM] * 4,
            out_specs=(ANY,) * 3,
            scratch_shapes=[pltpu.SemaphoreType.DMA((64,))],
            compiler_params=pltpu.CompilerParams(vmem_limit_bytes=12 * 2**20),
            name="store",
        )(*parts)
        return r_out, conv_out.transpose(0, 2, 3, 1), ssm_out.transpose(0, 1, 3, 2)

    cache_spec = P(None, ("dp", "tx"), "ty", None)
    in_specs = (P("dp", "tx"), P(None, "tx"), P(None, "tx", None, "ty"), P(None, "ty", None), P(None, "ty"), P(None, "ty", None), P(None, None, "ty"), P(None, "ty"), P(None, "ty", None), P(None, "ty"), P(None, "ty", "tx"), cache_spec, cache_spec)
    out_specs = (P("dp", "tx"), cache_spec, cache_spec)
    return jax.shard_map(local_step, mesh=mesh, in_specs=in_specs, out_specs=out_specs, check_vma=False)
```
